256 devices in a mesh: ctx: 16 (over z_hi, x, core), exp: 16 (over y, z_lo).
Axes of the slice: x: 4, y: 4, z: 8 (z_hi: 2, z_lo: 4; z = z_hi * 4 + z_lo), core: 2. Of those that a mesh axis runs over, the one named last changes fastest.
Arguments:
- q_nope: bfloat16 [1024, 128, 512], P('ctx', 'exp'), may hold values from -72 to 72
- q_rope: bfloat16 [1024, 8192], P('ctx', 'exp'), may hold values from -6 to 6
- cache_keys: bfloat16 [576, 2048], P(None, 'ctx'), may hold values from -6 to 6
- fresh_keys: bfloat16 [576, 1024], P(None, 'ctx'), may hold values from -6 to 6
- block_order: int32 [32], replicated, may hold values from 0 to 31, each once
- w_uv: bfloat16 [128, 512, 128], P('exp'), may hold values from -0.25 to 0.25
- w_out: bfloat16 [16384, 7168], P('exp', 'ctx'), may hold values from -0.046875 to 0.046875
- residual: bfloat16 [1024, 7168], P(('ctx', 'exp')), may hold values from -6 to 6
- norm_gain: float32 [7168], replicated, may hold values from 0.5 to 1.5
- router_weight: bfloat16 [7168, 16], replicated, may hold values from -0.0625 to 0.0625
- expert_ids: int32 [1024, 8], P(('ctx', 'exp')), may hold values from 0 to 15, all different within a row; in each aligned block of 4 rows (0 to 3, 4 to 7, ...) at most 3 rows name the same one
- w_gate: bfloat16 [16, 7168, 2048], P('exp', None, 'ctx'), may hold values from -0.0625 to 0.0625
- w_up: bfloat16 [16, 7168, 2048], P('exp', None, 'ctx'), may hold values from -0.0625 to 0.0625
- w_down: bfloat16 [16, 2048, 7168], P('exp', 'ctx'), may hold values from -0.125 to 0.125
Outputs:
- layer_out: bfloat16 [1024, 7168], P(('ctx', 'exp'))
The draws below stay inside these ranges and needn't reach their ends.
Inputs may be any that keep to these rules, and one draw needn't show every extreme that they name: A permutation: block j of the new tokens (32 rows) sits at positions 2048 + block_order[j] * 32 onward. `expert_ids`: each row names 8 different experts; the 4 rows of one device name no expert more than 3 times, and in some aligned block one expert exactly 3 times.
All inputs are finite; a program needn't handle non-finite values.
Results may differ from the reference program's by a relative error of at most 0.012.
Values may be sent and summed in bfloat16 or wider, within the bound.
A program may use at most 128 MiB of HBM per device.

```python
import math
import jax
import jax.numpy as jnp
import numpy as np
from jax import lax

D = 7168
HEADS = 128
LAT = 512
ROPE = 64
QKD = 192
VHD = 128
FF = 2048
TOP = 8
EXPERTS = 16
TOK_DEV = 4
KD = 576
FFS = 128
CAP = 3
BLK = 32
NBLK = 32
NEWTOK = 1024
CACHE = 2048


def latent_cache(key):
    baseline = jax.random.normal(jax.random.fold_in(key, 101), (KD, CACHE), jnp.float32)
    return jnp.clip(baseline, -6.0, 6.0)


def draw_cache_keys(key, part):
    return latent_cache(key).astype(jnp.bfloat16)


def draw_q_nope(key, part):
    queries = jnp.clip(jax.random.normal(jax.random.fold_in(key, 202), (NEWTOK, HEADS, LAT), jnp.float32), -6.0, 6.0)
    return queries.astype(jnp.bfloat16)


def steps_of(rng, dims, cuts, low, top_value):
    loudness = 1.0
    for position, parts in cuts:
        steps = jax.random.uniform(jax.random.fold_in(jax.random.fold_in(rng, 6), position), (parts,), jnp.float32, low / len(cuts), top_value / len(cuts))
        loudness = loudness * jnp.repeat(jnp.exp(steps), dims[position] // parts).reshape((-1,) + (1,) * (len(dims) - 1 - position))
    return loudness


def shared_out(own_key, own, number, rows, amount, top, limit, skew):
    sequence = jax.random.permutation(own_key, amount)
    crowded, common = load_shares(amount, rows * top, limit, skew, True), load_shares(amount, rows * top, limit, skew, False)
    places = jnp.arange(amount)

    def named(tallies, rotation):
        used = int((tallies > 0).sum())
        fixed = max(1, used // 4)
        moved = fixed + (places - fixed + rotation * (used - fixed)) % max(1, amount - fixed)
        return jnp.zeros((amount,), jnp.int32).at[sequence[jnp.where(places < fixed, places, moved)]].set(jnp.asarray(tallies, jnp.int32))

    tallies = jnp.where(number % 4 == 0, named(crowded, number // 4), named(common, number - number // 4 - 1))
    mixed = jax.random.permutation(jax.random.fold_in(own, 3), amount)
    source_of, sink = mixed[0:amount // 2 * 2:2], mixed[1:amount // 2 * 2:2]
    room = jnp.minimum(tallies[source_of] - 1, limit - tallies[sink]) // 2
    room = jnp.where((source_of == sequence[0]) | (sink == sequence[0]) | (tallies[sink] == 0), 0, jnp.maximum(room, 0))
    moved = jax.random.randint(jax.random.fold_in(own, 4), (amount // 2,), 0, 1 << 20) % (room + 1)
    tallies = tallies.at[source_of].add(-moved).at[sink].add(moved)
    items = jnp.searchsorted(jnp.cumsum(tallies), jnp.arange(rows * top), side="right").astype(jnp.int32)
    table = items.reshape(top, rows).T
    table = table[jax.random.permutation(jax.random.fold_in(own, 1), rows)]
    rotation = jax.random.randint(jax.random.fold_in(own, 2), (rows, 1), 0, top)
    return jnp.take_along_axis(table, (jnp.arange(top)[None, :] + rotation) % top, axis=1)


def load_shares(count, total, bound, slope, full):
    loads = [(1 << 20) // math.isqrt(grade ** slope) + 1 for grade in range(1, count + 1)]
    largest = bound if full else min(bound, max(-(-total // count), total * loads[0] // sum(loads)))
    least = 1 if total - largest >= count - 1 else 0
    given, spare = [largest] + [least] * (count - 1), total - largest - least * (count - 1)
    while spare > 0:
        candidates = [i for i in range(1, count) if given[i] < largest] or [i for i in range(1, count) if given[i] < bound]
        pool, remaining = sum([loads[i] for i in candidates]), spare
        for i in candidates:
            extra = min(bound - given[i], max(1, remaining * loads[i] // pool), spare)
            given[i] = given[i] + extra
            spare = spare - extra
    return np.array(given)


def centred(stream_key, dims, width, most, cuts=(), kind=jnp.bfloat16):
    values = jax.random.normal(stream_key, dims, jnp.float32) * width
    if len(cuts) > 0:
        values = steps_of(stream_key, dims, cuts, -0.22, 0.18) * values
    return jnp.clip(values, min=-most, max=most).astype(kind)


def setup_inputs(seed: int = 0) -> dict:
    key_of = jax.random.split(jax.random.key(seed), 15)
    q_nope = draw_q_nope(jax.random.fold_in(key_of[14], 71), 0)
    q_rope = centred(key_of[1], (NEWTOK, HEADS * ROPE), 1.0, 6.0, ((0, 16), (1, 16)))
    cache_keys = draw_cache_keys(jax.random.fold_in(key_of[14], 71), 0)
    fresh_keys = centred(key_of[3], (KD, NEWTOK), 1.0, 6.0, ((1, 16),))
    block_order = jax.random.permutation(key_of[4], NBLK).astype(jnp.int32)
    w_uv = centred(key_of[5], (HEADS, LAT, VHD), LAT ** -0.5, 0.25, ((0, 16),))
    w_out = centred(key_of[6], (HEADS * VHD, D), (HEADS * VHD) ** -0.5, 0.046875, ((0, 16), (1, 16)))
    residual = centred(key_of[7], (NEWTOK, D), 1.0, 6.0, ((0, 256),))
    norm_gain = jnp.clip(1.0 + 0.1 * jax.random.normal(key_of[8], (D,), jnp.float32), 0.5, 1.5)
    router_weight = centred(key_of[9], (D, EXPERTS), D ** -0.5, 0.0625)
    expert_ids_keys = jax.random.split(jax.random.fold_in(key_of[10], 1), NEWTOK // TOK_DEV)
    expert_ids_turns = jax.random.permutation(jax.random.fold_in(key_of[10], 3), NEWTOK // TOK_DEV)
    expert_ids = jax.vmap(lambda own, number: shared_out(jax.random.fold_in(key_of[10], 2), own, number, TOK_DEV, EXPERTS, TOP, CAP, 2))(expert_ids_keys, expert_ids_turns).reshape((NEWTOK, TOP))
    w_gate = centred(key_of[11], (EXPERTS, D, FF), D ** -0.5, 0.0625, ((0, 16), (2, 16)))
    w_up = centred(key_of[12], (EXPERTS, D, FF), D ** -0.5, 0.0625, ((0, 16), (2, 16)))
    w_down = centred(key_of[13], (EXPERTS, FF, D), FF ** -0.5, 0.125, ((0, 16), (1, 16)))
    return dict(q_nope=q_nope, q_rope=q_rope, cache_keys=cache_keys, fresh_keys=fresh_keys, block_order=block_order, w_uv=w_uv, w_out=w_out, residual=residual, norm_gain=norm_gain, router_weight=router_weight, expert_ids=expert_ids, w_gate=w_gate, w_up=w_up, w_down=w_down)


ROUTE_SCALE = 2.5
NORM_EPS = 1e-06

def block_position(row_index, block_order):
    blocks = row_index // BLK
    lookup = blocks[:, None] == jnp.arange(NBLK, dtype=jnp.int32)[None, :]
    leading = lax.optimization_barrier(jnp.sum(jnp.where(lookup, block_order[None, :], 0), axis=1))
    return (leading * BLK + row_index % BLK).astype(jnp.int32)

def reference(q_nope, q_rope, cache_keys, fresh_keys, block_order, w_uv, w_out, residual, norm_gain, router_weight, expert_ids, w_gate, w_up, w_down):
    keys = jnp.concatenate([cache_keys, fresh_keys], axis=1)
    query_pos = block_position(jnp.arange(NEWTOK, dtype=jnp.int32), block_order)
    key_pos = jnp.concatenate([jnp.full((CACHE,), -1, jnp.int32), query_pos])
    visible = key_pos[None, :] <= query_pos[:, None]
    scale = 1.0 / math.sqrt(QKD)
    latent_keys = keys[:LAT]
    rotary_keys = keys[LAT:]

    def one_head(inputs):
        query_lat, query_pe, w_head = inputs
        first_dot = jnp.dot(query_lat, latent_keys, preferred_element_type=jnp.float32)
        second_dot = jnp.dot(query_pe, rotary_keys, preferred_element_type=jnp.float32)
        scores = jnp.where(visible, (first_dot + second_dot) * scale, -jnp.inf)
        row_max = lax.optimization_barrier(jnp.max(scores, axis=1, keepdims=True))
        exponent = jnp.exp(scores - row_max)
        row_sum = lax.optimization_barrier(jnp.sum(exponent, axis=1, keepdims=True))
        latent = lax.dot_general(exponent.astype(jnp.bfloat16), latent_keys, (((1,), (1,)), ((), ())), preferred_element_type=jnp.float32) / row_sum
        return jnp.dot(latent, w_head.astype(jnp.float32), precision=lax.Precision.HIGHEST).astype(jnp.bfloat16)
    head_inputs = (jnp.transpose(q_nope, (1, 0, 2)), jnp.transpose(q_rope.reshape(NEWTOK, HEADS, ROPE), (1, 0, 2)), w_uv)
    head_out = lax.map(one_head, head_inputs)
    head_out = jnp.transpose(head_out, (1, 0, 2)).reshape(NEWTOK, HEADS * VHD)
    attention = jnp.dot(head_out, w_out, preferred_element_type=jnp.float32).astype(jnp.bfloat16)
    hidden = residual.astype(jnp.float32) + attention.astype(jnp.float32)
    mean_square = lax.optimization_barrier(jnp.mean(hidden * hidden, axis=1, keepdims=True))
    normed = (hidden * lax.rsqrt(mean_square + NORM_EPS) * norm_gain).astype(jnp.bfloat16)
    affinity = jax.nn.sigmoid(jnp.dot(normed, router_weight, preferred_element_type=jnp.float32))
    chosen = jnp.take_along_axis(affinity, expert_ids, axis=1)
    route = ROUTE_SCALE * chosen / lax.optimization_barrier(jnp.sum(chosen, axis=1, keepdims=True))
    onehot = expert_ids[:, :, None] == jnp.arange(EXPERTS, dtype=jnp.int32)[None, None, :]
    mixing = lax.optimization_barrier(jnp.sum(jnp.where(onehot, route[:, :, None], 0.0), axis=1))

    def one_expert(running, inputs):
        gate_matrix, up_matrix, down_matrix, mix_column = inputs
        gate = jnp.dot(normed, gate_matrix, preferred_element_type=jnp.float32)
        upward = jnp.dot(normed, up_matrix, preferred_element_type=jnp.float32)
        act = (jax.nn.silu(gate) * upward).astype(jnp.bfloat16)
        act_blocks = jnp.transpose(act.reshape(NEWTOK, FF // FFS, FFS), (1, 0, 2))
        down_blocks = down_matrix.reshape(FF // FFS, FFS, D)

        def add_block(accum, pair):
            block_out = jnp.dot(pair[0], pair[1], preferred_element_type=jnp.float32).astype(jnp.bfloat16)
            block_out = lax.optimization_barrier(block_out)
            return (accum + block_out.astype(jnp.float32), None)
        summed, ignored = lax.scan(add_block, jnp.zeros((NEWTOK, D), jnp.float32), (act_blocks, down_blocks))
        expert_out = lax.optimization_barrier(summed.astype(jnp.bfloat16)).astype(jnp.float32)
        return (running + mix_column[:, None] * expert_out, None)
    mixture, ignored = lax.scan(one_expert, jnp.zeros((NEWTOK, D), jnp.float32), (w_gate, w_up, w_down, mixing.T))
    return (hidden + mixture).astype(jnp.bfloat16)
```

```python
import functools
import math

import jax
import jax.numpy as jnp
from jax import lax
from jax.experimental import pallas as pl
from jax.experimental.pallas import tpu as pltpu
from jax.sharding import PartitionSpec as P

QKD = 192
ROUTE_SCALE = 2.5
NORM_EPS = 1e-06
MESH = pl.DeviceIdType.MESH
BF16 = jnp.bfloat16
F32 = jnp.float32
VMEM_LIMIT = 60 * 1024 * 1024
CHUNKS = 6
ROWS = 256
LOG_SCALE = math.log2(math.e) / math.sqrt(QKD)


def coords():
    c = lax.axis_index("ctx")
    e = lax.axis_index("exp")
    core = lax.rem(c, 2)
    x = lax.rem(lax.div(c, 2), 4)
    zh = lax.div(c, 8)
    y = lax.div(e, 4)
    zl = lax.rem(e, 4)
    return core, x, y, zh, zl


def device(core, x, y, z):
    return ((lax.div(z, 4) * 4 + x) * 2 + core, y * 4 + lax.rem(z, 4))


def one(v):
    return v + 1 - 2 * lax.rem(v, 2)


def two(v):
    return lax.rem(v + 2, 4)


def three(v):
    return 3 - v


def choose(i, table):
    value = table[0]
    for n in range(1, len(table)):
        value = jnp.where(i == n, table[n], value)
    return value


def swap(core, first, second):
    return first + core * (second - first), second + core * (first - second)


class Net:
    def __init__(self, send_sems, recv_sems):
        self.send_sems, self.recv_sems = send_sems, recv_sems
        self.count = 0
        self.sent = []

    def make(self, src, dst, dev):
        index = self.count
        self.count += 1
        return pltpu.make_async_remote_copy(
            src_ref=src,
            dst_ref=dst,
            send_sem=self.send_sems.at[index],
            recv_sem=self.recv_sems.at[index],
            device_id=dev,
            device_id_type=MESH,
        )

    def plan(self, src, dst, dev):
        copy = self.make(src, dst, dev)
        self.sent.append(copy)
        return copy

    def send(self, src, dst, dev):
        copy = self.plan(src, dst, dev)
        copy.start()
        return copy

    def drain(self):
        for copy in self.sent:
            copy.wait_send()


class Later:
    def __init__(self, **kwargs):
        self.kwargs = kwargs

    def start(self):
        pltpu.make_async_remote_copy(**self.kwargs).start()

    def wait_recv(self):
        pltpu.make_async_remote_copy(**self.kwargs).wait_recv()

    def wait_send(self):
        pltpu.make_async_remote_copy(**self.kwargs).wait_send()


def greet(peers, meanwhile):
    barrier = pltpu.get_barrier_semaphore()
    for peer in peers:
        pl.semaphore_signal(barrier, inc=1, device_id=peer, device_id_type=MESH)
    meanwhile()
    pl.semaphore_wait(barrier, len(peers))


class Layer:
    def __init__(self, refs, net):
        self.__dict__.update(refs)
        self.net = net
        self.core, self.x, self.y, self.zh, self.zl = coords()
        self.z = self.zh * 4 + self.zl
        self.e = self.y * 4 + self.zl
        self.a, self.b = swap(self.core, self.y, self.x)
        core, x, y, z = self.core, self.x, self.y, self.z
        z_far = (1 - self.zh) * 4 + self.zl
        self.partner = device(1 - core, x, y, z)
        self.x_peers = [device(core, lax.rem(x + d, 4), y, z) for d in range(1, 4)]
        self.y_peers = [device(core, x, lax.rem(y + d, 4), z) for d in range(1, 4)]
        self.z_peers = [device(core, x, y, lax.rem(z + d, 8)) for d in range(1, 8)]
        self.far_peers = [device(core, lax.rem(x + d, 4), y, z_far) for d in range(4)]

    def place(self, a_, b_, z_):
        y_, x_ = swap(self.core, a_, b_)
        return device(self.core, x_, y_, z_)

    def load(self, src, dst):
        copy = pltpu.make_async_copy(src, dst, self.local_sems.at[self.loads])
        self.loads += 1
        copy.start()
        return copy

    def start(self):
        self.loads = 0
        core, x, y, zh, zl = self.core, self.x, self.y, self.zh, self.zl
        me = zh * 4 + x
        own_cache = self.load(self.cache, self.cached.at[zh, x, core])
        own_fresh = self.load(self.fresh, self.newer.at[zh, x, core])
        self.own_rows = self.load(
            self.residual.at[:, pl.ds(pl.multiple_of(me * 896, 128), 896)], self.rows_in.at[me]
        )
        self.uv_load = self.load(self.w_uv, self.uv)
        self.wo_load = self.load(
            self.w_out, self.wo.at[pl.ds(pl.multiple_of(core * 448, 64), 448)]
        )
        self.moe_loads = [
            self.load(self.w_gate, self.w_all.at[0]),
            self.load(self.w_up, self.w_all.at[1]),
            self.load(self.w_down, self.wd.at[0]),
        ]
        peers = self.x_peers + self.y_peers + self.z_peers + self.far_peers[1:] + [self.partner]
        greet(peers, self.prepare_queries)
        own_cache.wait()
        own_fresh.wait()

    def prepare_queries(self):
        x, y, zh, zl = self.x, self.y, self.zh, self.zl
        lane = lax.broadcasted_iota(jnp.int32, (1, 128), 1)
        marks = jnp.zeros((1, 128), F32)
        for j in range(4):
            for n in range(8):
                marks += jnp.where(lane == self.ids[j, n] + 16 * j, 1.0, 0.0)
        self.marks[zh, x, y, zl] = marks
        @pl.loop(0, 8)
        def _(i):
            some = pl.ds(pl.multiple_of(i * 8, 8), 8)
            rows = pl.ds(pl.multiple_of(i * 64, 64), 64)
            self.q[rows, 0:512] = self.q_nope[some].astype(F32).reshape(64, 512).astype(BF16)

        for h in range(8):
            self.pe[pl.ds(h, 64, stride=8), 0:64] = self.q_rope[:, h * 64 : h * 64 + 64].astype(F32)
        self.q[:, 512:576] = self.pe[:, 0:64].astype(BF16)
        self.peak[...] = jnp.full((512, 128), -jnp.inf, F32)
        self.mass[...] = jnp.zeros((512, 128), F32)
        self.mean[...] = jnp.zeros((4, 512, 128), F32)
    def gather_and_attend(self):
        net = self.net
        core, x, y, zh, zl, z = self.core, self.x, self.y, self.zh, self.zl, self.z
        far = 1 - zh
        x1, x2, x3 = one(x), two(x), three(x)
        to_one, to_three = device(core, x1, y, z), device(core, x3, y, z)
        parts = ((self.cached, 0, 288), (self.cached, 288, 288), (self.newer, 0, 64))

        def whole(side, column, dev):
            refs = [r.at[side, column, core, pl.ds(at, size)] for r, at, size in parts]
            return [net.plan(ref, ref, dev) for ref in refs]

        def piece(side, column, late, dev):
            refs = [
                r.at[side, column, core, pl.ds(at + late * size // 2, size // 2)] for r, at, size in parts
            ]
            return [net.plan(ref, ref, dev) for ref in refs]

        def go(copies):
            for copy in copies:
                copy.start()

        def arrive(copies):
            for copy in copies:
                copy.wait_recv()

        edge = jnp.logical_or(zl == 0, zl == 3)
        z_out = lax.rem(z + 8 + jnp.where(zl == 0, -1, 1), 8)
        z_in = lax.rem(z + 8 + jnp.where(zl == 0, 1, -1), 8)
        z_copies, z_nexts = [], []
        for r, at, size in parts:
            near_ref = r.at[zh, x, core, pl.ds(at, size)]
            far_ref = r.at[far, x, core, pl.ds(at, size)]
            z_copies.append(net.make(near_ref, near_ref, device(core, x, y, z_out)))
            z_nexts.append(net.make(far_ref, far_ref, device(core, x, y, z_in)))

        @pl.when(edge)
        def _():
            for copy in z_copies:
                copy.start()

        near = whole(zh, x, to_one), whole(zh, x, to_three)
        near_pieces = piece(zh, x1, 0, to_three), piece(zh, x3, 1, to_one)
        share = whole(far, x, to_one), whole(far, x, to_three)
        far_pieces = piece(far, x1, 0, to_three), piece(far, x3, 1, to_one)
        gifts = [whole(side, c, self.partner) for side in (zh, far) for c in (x, x1, x3, x2)]
        go(near[0] + near[1] + gifts[0])
        row_copies = []
        me = zh * 4 + x
        for d in range(7):
            column, side = lax.rem(x + (d + 1) % 4, 4), zh if d < 3 else far
            there = side * 4 + column
            row_copies.append(
                net.send(
                    self.residual.at[:, pl.ds(pl.multiple_of(there * 896, 128), 896)],
                    self.rows_in.at[me],
                    device(core, column, y, side * 4 + zl),
                )
            )
        mark = self.marks.at[zh, x, y, zl]
        marks_z = [net.send(mark, mark, p) for p in self.z_peers]
        mark = self.marks.at[:, x, y]
        marks_x = [net.plan(mark, mark, p) for p in self.x_peers]
        mark = self.marks.at[:, :, y]
        marks_y = [net.plan(mark, mark, p) for p in self.y_peers]
        wo_here = self.wo.at[pl.ds(pl.multiple_of(core * 448, 64), 448)]
        weights = [
            net.plan(self.w_out, wo_here, self.partner),
            net.plan(self.w_gate, self.w_all.at[2], self.partner),
            net.plan(self.w_up, self.w_all.at[3], self.partner),
            net.plan(self.w_down, self.wd.at[1], self.partner),
        ]

        order, first = self.order, core + 2 * me

        def pick(index, length, table):
            out = jnp.zeros(index.shape, jnp.int32)
            for n in range(length):
                out += jnp.where(index == n, order[table + n], 0)
            return out

        @pl.loop(0, 8)
        def _(i):
            @pl.when(i == 0)
            def _():
                arrive(gifts[0])

            @pl.when(i == 1)
            def _():
                for n in range(3):
                    for m in range(2):
                        near[m][n].wait_recv()
                        go([near_pieces[m][n], gifts[1 + m][n]])

                    @pl.when(edge)
                    def _():
                        z_copies[n].wait_recv()
                        z_nexts[n].start()

                arrive(gifts[1])

            @pl.when(i == 2)
            def _():
                arrive(marks_z)
                go(marks_x)
                arrive(gifts[2])

            @pl.when(i == 3)
            def _():
                for n in range(3):
                    @pl.when(jnp.logical_not(edge))
                    def _():
                        z_nexts[n].wait_recv()

                    go([share[0][n], share[1][n], gifts[4][n]])
                arrive(near_pieces[0] + near_pieces[1])
                go(gifts[3])
                arrive(gifts[3])

            @pl.when(i == 4)
            def _():
                arrive(marks_x)
                go(marks_y)
                arrive(gifts[4])

            @pl.when(i == 5)
            def _():
                for n in range(3):
                    for m in range(2):
                        share[m][n].wait_recv()
                        go([far_pieces[m][n], gifts[5 + m][n]])
                arrive(gifts[5])

            @pl.when(i == 6)
            def _():
                arrive(gifts[6])

            @pl.when(i == 7)
            def _():
                arrive(far_pieces[0] + far_pieces[1])
                go(gifts[7] + weights)
                arrive(gifts[7])

            with jax.named_scope("p_block"):
                side = jnp.where(i < 4, zh, far)
                j = lax.rem(i, 4)
                column = jnp.where(j == 0, x, jnp.where(j == 1, x1, jnp.where(j == 2, x3, x2)))
                old = jnp.concatenate([self.cached[side, column, 0], self.cached[side, column, 1]], axis=1)
                new = self.newer[side, column].reshape(128, 576)
                last = (((1,), (1,)), ((), ()))
                self.score[:, 0:256] = jnp.dot(self.q[...], old, preferred_element_type=F32)
                self.score[:, 256:384] = lax.dot_general(self.q[...], new, last, preferred_element_type=F32)
                lane = lax.broadcasted_iota(jnp.int32, (1, 128), 1)
                table = (side * 4 + column) * 4
                key_pos = pick(lax.div(lane, 32), 4, table) * 32 + lax.rem(lane, 32)

                @pl.loop(0, 512 // ROWS)
                def _(r):
                    here = pl.ds(pl.multiple_of(r * ROWS, ROWS), ROWS)
                    row = r * ROWS + lax.broadcasted_iota(jnp.int32, (ROWS, 1), 0)
                    first_pos, last_pos = order[first * 2] * 32, order[first * 2 + 1] * 32
                    pos = jnp.where(row < 256, first_pos, last_pos) + lax.rem(lax.div(row, 8), 32)
                    parts = [self.score[here, n * 128 : n * 128 + 128] * LOG_SCALE for n in range(3)]
                    parts[2] = jnp.where(key_pos <= pos, parts[2], -jnp.inf)
                    before = self.peak[here]
                    top = jnp.maximum(jnp.maximum(parts[0], parts[1]), parts[2])
                    peak = jnp.maximum(before, jnp.max(top, axis=1, keepdims=True))
                    fade = jnp.exp2(before - peak)
                    self.peak[here] = peak
                    self.fade[here] = fade
                    parts = [jnp.exp2(part - peak) for part in parts]
                    self.mass[here] = self.mass[here] * fade + (parts[0] + parts[1] + parts[2])
                    for n in range(3):
                        self.weight[here, n * 128 : n * 128 + 128] = parts[n].astype(BF16)

                added = lax.dot_general(
                    self.weight[:, 0:256], old[:512], last, preferred_element_type=F32
                ) + jnp.dot(self.weight[:, 256:384], new[:, :512], preferred_element_type=F32)
                for n in range(4):
                    self.mean[n] = self.mean[n] * self.fade[...] + added[:, n * 128 : n * 128 + 128]

        self.row_copies, self.weights, self.marks_y = row_copies, weights, marks_y
        self.edge, self.z_sent = edge, z_copies + z_nexts
        with jax.named_scope("p_values"):
            self.uv_load.wait()
            for h in range(8):
                some = pl.ds(h, 64, stride=8)
                mass = jnp.sum(self.mass[some], axis=1, keepdims=True)
                latent = jnp.concatenate([self.mean[n, some] / mass for n in range(4)], axis=1)
                high = latent.astype(BF16)
                low = (latent - high.astype(F32)).astype(BF16)
                out = jnp.dot(high, self.uv[h], preferred_element_type=F32)
                out += jnp.dot(low, self.uv[h], preferred_element_type=F32)
                self.heads[zh, x, :, h * 128 : h * 128 + 128] = out.astype(BF16)

    def prepare(self):
        for copy in [self.own_rows, self.wo_load]:
            copy.wait()
        for copy in self.row_copies + self.weights[:1] + self.marks_y:
            copy.wait_recv()
        self.rows[...] = jnp.zeros((128, 896), BF16)
        for block in range(8):
            self.rows[block * 16 : block * 16 + 4] = self.rows_in[block]

        @pl.loop(0, 128)
        def _(o):
            oy, oz = lax.div(lax.rem(o, 16), 4), lax.rem(o, 4)
            self.owners[pl.ds(o, 1)] = self.marks[lax.div(o, 64), lax.rem(lax.div(o, 16), 4), oy, oz]

        self.total[...] = jnp.zeros_like(self.total)
        self.logit[...] = jnp.zeros_like(self.logit)
        self.square[...] = jnp.zeros_like(self.square)

    def project_and_gather(self):
        net = self.net
        core, x, y, zh, zl, z, e = self.core, self.x, self.y, self.zh, self.zl, self.z, self.e
        a, b, place = self.a, self.b, self.place
        z_peers, z_far = self.z_peers, (1 - self.zh) * 4 + self.zl
        x1, x3 = one(x), three(x)
        to_one, to_three = device(core, x1, y, z), device(core, x3, y, z)

        cuts = pl.ds(0, 32), pl.ds(32, 32)
        x_sides = to_one, to_three

        def fan_out(side, half):
            ref = self.heads.at[side, x, cuts[half]]
            first = net.send(ref, ref, x_sides[half])
            second = net.send(ref, ref, x_sides[1 - half])
            return (first, second) if half == 0 else (second, first)

        def forward(side, copies):
            passed = []
            for half in range(2):
                copies[half][half].wait_recv()
                ref = self.heads.at[side, (x1, x3)[half], cuts[half]]
                passed.append(net.send(ref, ref, x_sides[1 - half]))
            return passed

        def arrive(side, copies, passed):
            copies[0][1].wait_recv()
            copies[1][0].wait_recv()
            for copy in passed:
                copy.wait_recv()

        def project(side):
            row = lax.broadcasted_iota(jnp.int32, (256, 128), 0) + side * 256
            col = lax.broadcasted_iota(jnp.int32, (256, 128), 1)
            pick = (row == lax.div(col, 16) * 64 + e * 4 + lax.rem(col, 16)) & (lax.rem(col, 16) < 4)
            pick = jnp.where(pick, 1.0, 0.0).astype(BF16)
            lhs = self.heads[side].reshape(256, 1024)
            for start, width in ((0, 256), (256, 256), (512, 256), (768, 128)):
                cols = pl.ds(start, width)
                block = lax.dot_general(
                    lhs, self.wo[cols], (((1,), (1,)), ((), ())), preferred_element_type=F32
                )
                block += jnp.dot(pick, self.rows[:, cols], preferred_element_type=F32)
                self.part[pl.ds(side * 2, 2), :, :, cols] = block.astype(BF16).reshape(2, 4, 32, width)

        with jax.named_scope("p_heads"):
            far_copies = []
            for half in range(2):
                ref = self.heads.at[zh, x, cuts[half]]
                far_copies.append(net.send(ref, ref, device(core, x, y, z_far)))
            near = fan_out(zh, 0), fan_out(zh, 1)
            self.prepare()
            near_passed = forward(zh, near)
            far = []
            for half in range(2):
                far_copies[half].wait_recv()
                far.append(fan_out(1 - zh, half))
        with jax.named_scope("p_near"):
            arrive(zh, near, near_passed)
            project(zh)
        with jax.named_scope("p_far"):
            far_passed = forward(1 - zh, far)
            arrive(1 - zh, far, far_passed)
            project(1 - zh)

        y1, y2, y3 = one(y), two(y), three(y)
        up, down = device(core, x, y1, z), device(core, x, y3, z)
        lo, hi = pl.ds(0, 2), pl.ds(2, 2)
        with jax.named_scope("p_sum_y"):
            s10 = net.send(self.part.at[y2, lo], self.y_in.at[0, 0], up)
            s20 = net.send(self.part.at[y2, hi], self.y_in.at[1, 0], down)
            s11 = net.send(self.part.at[y1, lo], self.y_in.at[0, 1], up)
            s21 = net.send(self.part.at[y3, hi], self.y_in.at[1, 1], down)
            s10.wait_recv()
            self.part[y3, lo] = (self.part[y3, lo].astype(F32) + self.y_in[0, 0].astype(F32)).astype(BF16)
            t1 = net.send(self.part.at[y3, lo], self.y_last.at[0], down)
            s20.wait_recv()
            self.part[y1, hi] = (self.part[y1, hi].astype(F32) + self.y_in[1, 0].astype(F32)).astype(BF16)
            t2 = net.send(self.part.at[y1, hi], self.y_last.at[1], up)
            s11.wait_recv()
            t1.wait_recv()
            self.part[y, lo] = (
                self.part[y, lo].astype(F32) + self.y_in[0, 1].astype(F32) + self.y_last[0].astype(F32)
            ).astype(BF16)
            s21.wait_recv()
            t2.wait_recv()
            self.part[y, hi] = (
                self.part[y, hi].astype(F32) + self.y_in[1, 1].astype(F32) + self.y_last[1].astype(F32)
            ).astype(BF16)
        with jax.named_scope("p_sum_z"):
            line = []
            for d in range(1, 4):
                there = lax.rem(zl + d, 4)
                line.append(
                    net.send(self.part.at[y, there], self.z_parts.at[d - 1], device(core, x, y, zh * 4 + there))
                )
            for copy in line:
                copy.wait_recv()
            hidden = self.part[y, zl].astype(F32)
            for d in range(3):
                hidden += self.z_parts[d].astype(F32)
            self.buf[a, b, z] = hidden[:, :768].astype(BF16)
        self.slim[z, a, b] = hidden[:, 768:].astype(BF16)

        with jax.named_scope("p_gather"):
            self.gather_rows()

    def gather_rows(self):
        net = self.net
        core, z = self.core, self.z
        a, b, place = self.a, self.b, self.place
        a1, a2, a3 = one(a), two(a), three(a)
        b1, b2, b3 = one(b), two(b), three(b)
        a_one, a_three = place(a1, b, z), place(a3, b, z)
        b_one, b_three = place(a, b1, z), place(a, b3, z)
        front, back = pl.ds(0, 4), pl.ds(4, 4)
        ref = self.buf.at[a, b, z]
        low, high = pl.ds(0, 16), pl.ds(16, 16)
        slim = self.slim
        slim_b = [net.send(slim.at[z, a, b], slim.at[z, a, b], p) for p in (b_one, b_three)]
        by_z = {d: net.send(ref, ref, self.z_peers[d - 1]) for d in (2, 6, 1, 7)}

        def fan(z_):
            ref = self.buf.at[a, b, z_]
            return [net.send(ref, ref, p) for p in (b_one, b_three, a_one, a_three)]

        def farther(d, hop, rows):
            by_z[d].wait_recv()
            z_ = lax.rem(z + 8 - d, 8)
            ref, part = self.buf.at[a, b, z_], self.buf.at[a, b, z_, rows]
            return net.send(ref, ref, self.z_peers[hop - 1]), net.send(part, part, self.z_peers[2 * hop % 8 - 1])

        with jax.named_scope("p_fan"):
            fans = [fan(z)]
            slim_b[0].wait_recv()
            ref = slim.at[z, a, b1, low]
            slim_more = [net.send(ref, ref, b_three)]
            slim_b[1].wait_recv()
            ref = slim.at[z, a, b3, high]
            slim_more.append(net.send(ref, ref, b_one))
            by_z[3], low_half = farther(2, 1, low)
            by_z[5], high_half = farther(6, 7, high)
            for d in (1, 7):
                by_z[d].wait_recv()
                fans.append(fan(lax.rem(z + 8 - d, 8)))
            for copy in slim_more:
                copy.wait_recv()
            ref = slim.at[z, a]
            slim_a = [net.send(ref, ref, p) for p in (a_one, a_three)]
            fans.append(fan(lax.rem(z + 6, 8)))
            fans.append(fan(lax.rem(z + 2, 8)))
            for d in (3, 5):
                by_z[d].wait_recv()
                fans.append(fan(lax.rem(z + 8 - d, 8)))
            low_half.wait_recv()
            high_half.wait_recv()
            fans.append(fan(lax.rem(z + 4, 8)))
            refs = slim.at[z, a1, pl.ds(0, 2)], slim.at[z, a3, pl.ds(2, 2)]
            slim_halves = [net.plan(ref, ref, dev) for ref, dev in zip(refs, (a_three, a_one))]
            slim_z = {d: net.plan(slim.at[z], slim.at[z], self.z_peers[d - 1]) for d in (2, 6, 1, 7)}
            slim_far = {}
            for d, hop, late in ((2, 1, 0), (6, 7, 2)):
                z_ = lax.rem(z + 8 - d, 8)
                part = slim.at[z_, pl.ds(late, 2)]
                slim_far[d] = (
                    net.plan(slim.at[z_], slim.at[z_], self.z_peers[hop - 1]),
                    net.plan(part, part, self.z_peers[2 * hop % 8 - 1]),
                )

        def spread(column):
            ref = self.buf.at[a, column]
            return [net.plan(ref, ref, p) for p in (a_one, a_three)]

        def halves(column):
            ref, other = self.buf.at[a1, column, front], self.buf.at[a3, column, back]
            return [net.plan(ref, ref, a_three), net.plan(other, other, a_one)]

        ref, other = self.buf.at[a, b1, front], self.buf.at[a, b3, back]
        b_halves = [net.plan(ref, ref, b_three), net.plan(other, other, b_one)]
        columns = (b, b1, b3, b2)
        spreads = [None] + [spread(column) for column in columns[1:]]
        passed = [halves(column) for column in columns]

        def go(*copies):
            for copy in copies:
                copy.start()

        def arrive(*copies):
            for copy in copies:
                copy.wait_recv()

        def pass_on(n):
            if n == 0:
                arrive(*[f[2] for f in fans])
                go(passed[0][0])
                arrive(*[f[3] for f in fans])
                go(passed[0][1])
            else:
                arrive(spreads[n][0])
                go(passed[n][0])
                arrive(spreads[n][1])
                go(passed[n][1])

        def first_sides():
            arrive(*slim_halves)
            go(*slim_z.values())
            arrive(*[f[0] for f in fans])
            go(b_halves[0], *spreads[1])
            arrive(*[f[1] for f in fans])
            go(b_halves[1], *spreads[2])

        def far_column():
            arrive(*b_halves)
            go(*spreads[3])
            for d in (2, 6):
                arrive(slim_z[d])
                go(*slim_far[d])

        def slim_products():
            arrive(slim_z[1], slim_z[7], *slim_far[2], *slim_far[6])

            @pl.loop(0, 8)
            def _(z_):
                side, row_z = lax.div(z_, 4), lax.rem(z_, 4)
                columns, weights, gains, routers = [], [], [], []
                for col_x in range(4):
                    features = pl.ds(pl.multiple_of((side * 4 + col_x) * 896 + 768, 128), 128)
                    rows = []
                    for row_y in range(4):
                        aa, bb = swap(core, row_y, col_x)
                        rows.append(slim[z_, aa, bb])
                    columns.append(jnp.concatenate(rows, axis=0))
                    weights.append(jnp.concatenate([self.w_all[n, features] for n in range(4)], axis=1))
                    gains.append(self.gain[:, features])
                    routers.append(self.router[:, features])
                piece = jnp.concatenate(columns, axis=1).astype(F32)
                square = jnp.sum(piece * piece, axis=1, keepdims=True)
                scaled = (piece * jnp.concatenate(gains, axis=1)).astype(BF16)
                total = jnp.dot(scaled, jnp.concatenate(weights, axis=0), preferred_element_type=F32)
                logit = lax.dot_general(
                    scaled, jnp.concatenate(routers, axis=1), (((1,), (1,)), ((), ())),
                    preferred_element_type=F32,
                )
                for row_y in range(4):
                    here = pl.ds(pl.multiple_of(row_y * 128 + row_z * 32, 32), 32)
                    some = slice(row_y * 32, row_y * 32 + 32)
                    self.square[here] += jnp.broadcast_to(square[some], (32, 128))
                    self.total[here] += total[some]
                    self.logit[here] += logit[some]

            arrive(*passed[1])

        def weights_here():
            for n in range(2):
                slim_a[n].wait_recv()
                slim_halves[n].start()
            for load in self.moe_loads:
                load.wait()
            for copy in self.weights[1:]:
                copy.wait_recv()

        steps = {
            0: weights_here,
            1: first_sides,
            3: lambda: pass_on(0),
            5: far_column,
            6: lambda: pass_on(1),
            8: lambda: arrive(*passed[0]),
            9: lambda: pass_on(2),
            11: slim_products,
            12: lambda: pass_on(3),
            14: lambda: arrive(*passed[2]),
            15: lambda: arrive(*passed[3]),
        }
        order_a = (a, a, a, a1, a3, a, a1, a3, a2, a1, a3, a2, a1, a3, a2, a2)
        order_b = (b, b1, b3, b, b, b2, b1, b1, b, b3, b3, b1, b2, b2, b3, b2)

        @pl.loop(0, 16)
        def _(i):
            for n, step in steps.items():
                pl.when(i == n)(step)
            with jax.named_scope("p_unit"):
                aa, bb = choose(i, order_a), choose(i, order_b)
                row_y, col_x = swap(core, aa, bb)
                here = pl.ds(pl.multiple_of(row_y * 128, 128), 128)
                for side in range(2):
                    features = pl.ds(pl.multiple_of((side * 4 + col_x) * 896, 128), 768)
                    piece = self.buf[aa, bb, pl.ds(side * 4, 4)].reshape(128, 768).astype(F32)
                    self.square[here] += jnp.broadcast_to(
                        jnp.sum(piece * piece, axis=1, keepdims=True), (128, 128)
                    )
                    scaled = (piece * self.gain[:, features]).astype(BF16)
                    weights = jnp.concatenate([self.w_all[n, features] for n in range(4)], axis=1)
                    self.total[here] += jnp.dot(scaled, weights, preferred_element_type=F32)
                    self.logit[here] += lax.dot_general(
                        scaled, self.router[:, features], (((1,), (1,)), ((), ())),
                        preferred_element_type=F32,
                    )

    def experts(self):
        core, e = self.core, self.e

        @pl.loop(0, 2)
        def _(side):
            here = pl.ds(pl.multiple_of(side * 256, 256), 256)
            scale = lax.rsqrt(self.square[here] * (1.0 / 7168.0) + NORM_EPS)
            row = lax.broadcasted_iota(jnp.int32, (256, 128), 0)
            col = lax.broadcasted_iota(jnp.int32, (256, 128), 1)
            owner = jnp.where(col == side * 64 + lax.div(row, 4), 1.0, 0.0)
            named = jnp.dot(owner, self.owners[...], preferred_element_type=F32)
            mask = jnp.zeros((256, 16), F32)
            for n in range(4):
                mask += jnp.where(lax.rem(row[:, :16], 4) == n, named[:, n * 16 : n * 16 + 16], 0.0)
            chosen = mask * jax.nn.sigmoid(self.logit[here] * scale[:, :16])
            lane = lax.broadcasted_iota(jnp.int32, (256, 16), 1)
            named = jnp.sum(jnp.where(lane == e, chosen, 0.0), axis=1, keepdims=True)
            mix = ROUTE_SCALE * named / jnp.sum(chosen, axis=1, keepdims=True)
            for i in range(2):
                gate = self.total[here, i * 256 : i * 256 + 128] * scale
                upward = self.total[here, i * 256 + 128 : i * 256 + 256] * scale
                act = (gate * jax.nn.sigmoid(gate) * upward * mix).astype(BF16)
                act = act.reshape(4, 4, 16, 128)
                for bx in range(4):
                    for by in range(4):
                        aa, bb = swap(core, by, bx)
                        self.act[aa, bb, side, :, i * 128 : i * 128 + 128] = act[bx, by]

    def own_hidden(self):
        owner = (self.zh * 4 + self.x) * 2 + lax.div(self.e, 8)
        oy, oz = lax.div(owner, 4), lax.rem(owner, 4)
        row = lax.broadcasted_iota(jnp.int32, (16, 32), 0)
        col = lax.broadcasted_iota(jnp.int32, (16, 32), 1)
        mine = jnp.where((col == lax.rem(self.e, 8) * 4 + row) & (row < 4), 1.0, 0.0).astype(BF16)
        for block in range(8):
            aa, bb = swap(self.core, oy, block % 4)
            rows = self.buf[aa, bb, block // 4 * 4 + oz]
            self.own[:, block * 896 : block * 896 + 768] = jnp.dot(
                mine, rows, preferred_element_type=F32
            )
            rows = self.slim[block // 4 * 4 + oz, aa, bb]
            self.own[:, block * 896 + 768 : block * 896 + 896] = jnp.dot(
                mine, rows, preferred_element_type=F32
            )

    def mix_down(self):
        net = self.net
        z = self.z
        a, b, place = self.a, self.b, self.place
        a1, a2, a3 = one(a), two(a), three(a)
        b1, b2, b3 = one(b), two(b), three(b)
        a_up, a_down = place(a1, b, z), place(a3, b, z)
        b_up, b_down = place(a, b1, z), place(a, b3, z)
        base, each = net.count, 19
        net.count += each * CHUNKS

        def copies(g):
            found = []

            def add(src, dst, dev):
                index = base + g * each + len(found)
                found.append(Later(
                    src_ref=src, dst_ref=dst, send_sem=net.send_sems.at[index],
                    recv_sem=net.recv_sems.at[index], device_id=dev, device_id_type=MESH,
                ))

            add(self.prod.at[0, g, a2], self.a_in.at[0, g, 0], a_up)
            add(self.prod.at[1, g, a2], self.a_in.at[1, g, 0], a_down)
            add(self.prod.at[0, g, a1], self.a_in.at[0, g, 1], a_up)
            add(self.prod.at[1, g, a3], self.a_in.at[1, g, 1], a_down)
            add(self.prod.at[0, g, a3], self.a_last.at[0, g], a_down)
            add(self.prod.at[1, g, a1], self.a_last.at[1, g], a_up)
            add(self.prod.at[0, g, a, b2], self.b_in.at[0, g, 0], b_up)
            add(self.prod.at[1, g, a, b2], self.b_in.at[1, g, 0], b_down)
            add(self.prod.at[0, g, a, b1], self.b_in.at[0, g, 1], b_up)
            add(self.prod.at[1, g, a, b3], self.b_in.at[1, g, 1], b_down)
            add(self.prod.at[0, g, a, b3], self.b_last.at[0, g], b_down)
            add(self.prod.at[1, g, a, b1], self.b_last.at[1, g], b_up)
            for d in range(1, 8):
                add(self.pack.at[g, d], self.z_in.at[g, d - 1], self.z_peers[d - 1])
            return found

        def merge(half, g, index, *sources):
            @pl.loop(0, 4)
            def _(r):
                value = self.prod[half, g, index, r].astype(F32)
                for source in sources:
                    value += source[r].astype(F32)
                self.prod[half, g, index, r] = value.astype(BF16)

        def add_in(half, g, index, *sources):
            value = self.prod[half, g, a, index].astype(F32)
            for source in sources:
                value += source[...].astype(F32)
            self.prod[half, g, a, index] = value.astype(BF16)

        def products(g):
            c = copies(g)

            @pl.loop(0, 8)
            def _(n):
                half = lax.rem(n, 2)
                index = choose(n, (a2, a2, a1, a3, a3, a1, a, a))
                cols = pl.ds(pl.multiple_of(half * 3584 + g * 512, 512), 512)
                block = jnp.dot(
                    self.act[index].reshape(128, 256), self.wd[:, :, cols].reshape(256, 512),
                    preferred_element_type=F32,
                )
                self.prod[half, g, index] = block.astype(BF16).reshape(4, 32, 512)
                for k in range(4):
                    pl.when(n == k)(c[k].start)

        def second(g):
            c = copies(g)
            c[0].wait_recv()
            merge(0, g, a3, self.a_in.at[0, g, 0])
            c[4].start()
            c[1].wait_recv()
            merge(1, g, a1, self.a_in.at[1, g, 0])
            c[5].start()

        def third(g):
            c = copies(g)
            c[2].wait_recv()
            c[4].wait_recv()
            merge(0, g, a, self.a_in.at[0, g, 1], self.a_last.at[0, g])
            c[6].start()
            c[8].start()
            c[3].wait_recv()
            c[5].wait_recv()
            merge(1, g, a, self.a_in.at[1, g, 1], self.a_last.at[1, g])
            c[7].start()
            c[9].start()

        def fourth(g):
            c = copies(g)
            c[6].wait_recv()
            add_in(0, g, b3, self.b_in.at[0, g, 0])
            c[10].start()
            c[7].wait_recv()
            add_in(1, g, b1, self.b_in.at[1, g, 0])
            c[11].start()

        def fifth(g):
            c = copies(g)
            c[8].wait_recv()
            c[10].wait_recv()
            add_in(0, g, b, self.b_in.at[0, g, 1], self.b_last.at[0, g])
            c[9].wait_recv()
            c[11].wait_recv()
            add_in(1, g, b, self.b_in.at[1, g, 1], self.b_last.at[1, g])
            value = jnp.zeros((128, 256), F32)
            for q in range(4):
                rows = self.prod[q // 2, g, a, b, :, q % 2 * 256 : q % 2 * 256 + 256]
                value += jnp.dot(self.picks[q], rows, preferred_element_type=F32)
            self.pack[g] = value.astype(BF16).reshape(8, 16, 256)
            for d in range(7):
                c[12 + d].start()

        def last(g):
            c = copies(g)
            result = self.pack[g, 0].astype(F32)
            for d in range(7):
                c[12 + d].wait_recv()
                result += self.z_in[g, d].astype(F32)
            for q in range(4):
                start = q // 2 * 3584 + q % 2 * 256 + g * 512
                cols = pl.ds(pl.multiple_of(start, 256), 256)
                self.out[:, cols] = (result[q * 4 : q * 4 + 4] + self.own[0:4, cols]).astype(BF16)
            for copy in c:
                copy.wait_send()

        v = {}
        ups = (a_up, a_down)
        b_peers = [place(a, lax.rem(b + d, 4), z) for d in range(1, 4)]
        v["z"] = [net.plan(self.v_prod.at[d], self.v_z.at[d - 1], self.z_peers[d - 1]) for d in range(1, 8)]
        v["first"] = [
            net.plan(self.v_sum.at[half, index], self.v_a.at[half, n], ups[half])
            for half, n, index in ((0, 0, a2), (1, 0, a2), (0, 1, a1), (1, 1, a3))
        ]
        v["second"] = [
            net.plan(self.v_sum.at[half, index], self.v_last.at[half], ups[1 - half])
            for half, index in ((0, a3), (1, a1))
        ]
        v["b"] = [net.plan(self.v_pack.at[d], self.v_b.at[d - 1], b_peers[d - 1]) for d in range(1, 4)]

        def v_products():
            row = lax.broadcasted_iota(jnp.int32, (256, 256), 0)
            col = lax.broadcasted_iota(jnp.int32, (256, 256), 1)
            source = lax.rem(lax.div(row, 4), 16) * 16 + lax.div(row, 64) * 4 + lax.rem(row, 4)
            order = jnp.where(col == source, 1.0, 0.0).astype(BF16)
            for side in range(2):
                rows = jnp.dot(order, self.act[:, :, side].reshape(256, 256), preferred_element_type=F32)
                self.act_z[pl.ds(side * 4, 4)] = rows.astype(BF16).reshape(4, 64, 256)

            @pl.loop(0, 8)
            def _(n):
                d = choose(n, (4, 3, 5, 2, 6, 1, 7, 0))
                for half in range(2):
                    start = half * 3584 + CHUNKS * 512
                    block = jnp.dot(
                        self.act_z[lax.rem(z + d, 8)], self.wd[:, :, start : start + 512].reshape(256, 512),
                        preferred_element_type=F32,
                    )
                    self.v_prod[d, :, half * 512 : half * 512 + 512] = block.astype(BF16)
                for k in range(1, 8):
                    pl.when(d == k)(v["z"][k - 1].start)

        def v_first():
            for copy in v["z"]:
                copy.wait_recv()
            for half in range(2):
                cols = pl.ds(half * 512, 512)
                value = self.v_prod[0, :, cols].astype(F32)
                for d in range(7):
                    value += self.v_z[d, :, cols].astype(F32)
                self.v_sum[half] = value.astype(BF16).reshape(4, 16, 512)
            for copy in v["first"]:
                copy.start()

        def v_add(half, index, *sources):
            value = self.v_sum[half, index].astype(F32)
            for source in sources:
                value += source[...].astype(F32)
            self.v_sum[half, index] = value.astype(BF16)

        def v_second():
            for half, index in ((0, a3), (1, a1)):
                v["first"][half].wait_recv()
                v_add(half, index, self.v_a.at[half, 0])
                v["second"][half].start()

        def v_third():
            for half in range(2):
                v["first"][2 + half].wait_recv()
                v["second"][half].wait_recv()
                v_add(half, a, self.v_a.at[half, 1], self.v_last.at[half])
            row = lax.broadcasted_iota(jnp.int32, (64, 16), 0)
            col = lax.broadcasted_iota(jnp.int32, (64, 16), 1)
            there = lax.rem(b + lax.div(row, 16), 4)
            value = jnp.zeros((64, 256), F32)
            for q in range(4):
                hit = (col == there * 4 + lax.rem(row, 4)) & (lax.rem(lax.div(row, 4), 4) == q)
                hit = jnp.where(hit, 1.0, 0.0).astype(BF16)
                rows = self.v_sum[q // 2, a, :, q % 2 * 256 : q % 2 * 256 + 256]
                value += jnp.dot(hit, rows, preferred_element_type=F32)
            self.v_pack[...] = value.astype(BF16).reshape(4, 16, 256)
            for copy in v["b"]:
                copy.start()

        def v_finish():
            result = self.v_pack[0].astype(F32)
            for d in range(3):
                v["b"][d].wait_recv()
                result += self.v_b[d].astype(F32)
            for q in range(4):
                start = q // 2 * 3584 + q % 2 * 256 + CHUNKS * 512
                cols = slice(start, start + 256)
                self.out[:, cols] = (result[q * 4 : q * 4 + 4] + self.own[0:4, cols]).astype(BF16)

        row = lax.broadcasted_iota(jnp.int32, (128, 32), 0)
        col = lax.broadcasted_iota(jnp.int32, (128, 32), 1)
        there = lax.rem(z + lax.div(row, 16), 8)
        for q in range(4):
            hit = (col == there * 4 + lax.rem(row, 4)) & (lax.rem(lax.div(row, 4), 4) == q)
            self.picks[q] = jnp.where(hit, 1.0, 0.0).astype(BF16)
        stages = (products, second, third, fourth, fifth, last)

        @pl.loop(0, CHUNKS + len(stages) - 1)
        def _(t):
            for n, stage in enumerate(stages):
                g = t - n

                @pl.when((g >= 0) & (g < CHUNKS))
                def _():
                    with jax.named_scope("p_stage%d" % n):
                        stage(g)

            @pl.when(t == 1)
            def _():
                with jax.named_scope("p_v0"):
                    v_products()
                self.own_hidden()

            for n, stage in enumerate((v_first, v_second, v_third, v_finish)):
                @pl.when(t == 7 + n)
                def _():
                    with jax.named_scope("p_v%d" % (n + 1)):
                        stage()

    def finish(self):
        @pl.when(self.edge)
        def _():
            for copy in self.z_sent:
                copy.wait_send()

        self.net.drain()


ANY = pl.BlockSpec(memory_space=pl.ANY)
VM = pl.BlockSpec(memory_space=pltpu.VMEM)
SM = pl.BlockSpec(memory_space=pltpu.SMEM)
DMA = pltpu.SemaphoreType.DMA
INPUTS = (
    ("q_nope", VM), ("q_rope", VM), ("cache", ANY), ("fresh", ANY), ("order", SM), ("w_uv", ANY),
    ("w_out", ANY), ("residual", ANY), ("gain", VM), ("router", VM), ("ids", SM), ("w_gate", ANY),
    ("w_up", ANY), ("w_down", ANY),
)
SCRATCH = (
    ("cached", (2, 4, 2, 576, 128), BF16),
    ("newer", (2, 4, 2, 64, 576), BF16),
    ("rows_in", (8, 4, 896), BF16),
    ("rows", (128, 896), BF16),
    ("marks", (2, 4, 4, 4, 1, 128), F32),
    ("owners", (128, 128), F32),
    ("uv", (8, 512, 128), BF16),
    ("wo", (896, 1024), BF16),
    ("w_all", (4, 7168, 128), BF16),
    ("wd", (2, 128, 7168), BF16),
    ("q", (512, 576), BF16),
    ("pe", (512, 128), F32),
    ("score", (512, 384), F32),
    ("weight", (512, 384), BF16),
    ("peak", (512, 128), F32),
    ("mass", (512, 128), F32),
    ("mean", (4, 512, 128), F32),
    ("fade", (512, 128), F32),
    ("heads", (2, 4, 64, 1024), BF16),
    ("part", (4, 4, 32, 896), BF16),
    ("y_in", (2, 2, 2, 32, 896), BF16),
    ("y_last", (2, 2, 32, 896), BF16),
    ("z_parts", (3, 32, 896), BF16),
    ("buf", (4, 4, 8, 32, 768), BF16),
    ("slim", (8, 4, 4, 32, 128), BF16),
    ("total", (512, 512), F32),
    ("logit", (512, 16), F32),
    ("square", (512, 128), F32),
    ("act", (4, 4, 2, 16, 256), BF16),
    ("own", (16, 7168), F32),
    ("prod", (2, CHUNKS, 4, 4, 32, 512), BF16),
    ("a_in", (2, CHUNKS, 2, 4, 32, 512), BF16),
    ("a_last", (2, CHUNKS, 4, 32, 512), BF16),
    ("b_in", (2, CHUNKS, 2, 32, 512), BF16),
    ("b_last", (2, CHUNKS, 32, 512), BF16),
    ("act_z", (8, 64, 256), BF16),
    ("v_prod", (8, 64, 1024), BF16),
    ("v_z", (7, 64, 1024), BF16),
    ("v_sum", (2, 4, 16, 512), BF16),
    ("v_a", (2, 2, 16, 512), BF16),
    ("v_last", (2, 16, 512), BF16),
    ("v_pack", (4, 16, 256), BF16),
    ("v_b", (3, 16, 256), BF16),
    ("picks", (4, 128, 32), BF16),
    ("pack", (CHUNKS, 8, 16, 256), BF16),
    ("z_in", (CHUNKS, 7, 16, 256), BF16),
)
COPIES = 400


def layer_kernel(*refs):
    names = [n for n, _ in INPUTS] + ["out"] + [n for n, *_ in SCRATCH]
    layer = Layer(dict(zip(names, refs)), Net(*refs[-2:]))
    layer.local_sems = refs[-3]
    with jax.named_scope("p_start"):
        layer.start()
    with jax.named_scope("p_attend"):
        layer.gather_and_attend()
    with jax.named_scope("p_project"):
        layer.project_and_gather()
    with jax.named_scope("p_experts"):
        layer.experts()
    with jax.named_scope("p_down"):
        layer.mix_down()
    layer.finish()


def body(
    q_nope, q_rope, cache_keys, fresh_keys, block_order, w_uv, w_out, residual,
    norm_gain, router_weight, expert_ids, w_gate, w_up, w_down,
):
    return pl.pallas_call(
        layer_kernel,
        out_shape=jax.ShapeDtypeStruct((4, 7168), BF16),
        in_specs=[spec for _, spec in INPUTS],
        out_specs=VM,
        scratch_shapes=[pltpu.VMEM(dims, kind) for _, dims, kind in SCRATCH]
        + [DMA((8,)), DMA((COPIES,)), DMA((COPIES,))],
        compiler_params=pltpu.CompilerParams(
            collective_id=0, has_side_effects=True, vmem_limit_bytes=VMEM_LIMIT
        ),
    )(
        q_nope, q_rope, cache_keys, fresh_keys.T, block_order, w_uv, w_out.T, residual,
        norm_gain.reshape(1, 7168), router_weight.T, expert_ids, w_gate[0], w_up[0], w_down[0],
    )


def solution(mesh):
    return jax.shard_map(
        body,
        mesh=mesh,
        in_specs=(
            P("ctx", "exp", None),
            P("ctx", "exp"),
            P(None, "ctx"),
            P(None, "ctx"),
            P(),
            P("exp", None, None),
            P("exp", "ctx"),
            P(("ctx", "exp"), None),
            P(),
            P(),
            P(("ctx", "exp"), None),
            P("exp", None, "ctx"),
            P("exp", None, "ctx"),
            P("exp", "ctx", None),
        ),
        out_specs=P(("ctx", "exp"), None),
        check_vma=False,
    )
```

```python
import functools
import math

import jax
import jax.numpy as jnp
from jax import lax
from jax.experimental import pallas as pl
from jax.experimental.pallas import tpu as pltpu
from jax.sharding import PartitionSpec as P

QKD = 192
ROUTE_SCALE = 2.5
NORM_EPS = 1e-06
MESH = pl.DeviceIdType.MESH
BF16 = jnp.bfloat16
F32 = jnp.float32
VMEM_LIMIT = 60 * 1024 * 1024
CHUNKS = 6
ROWS = 256
LOG_SCALE = math.log2(math.e) / math.sqrt(QKD)


def coords():
    c = lax.axis_index("ctx")
    e = lax.axis_index("exp")
    core = lax.rem(c, 2)
    x = lax.rem(lax.div(c, 2), 4)
    zh = lax.div(c, 8)
    y = lax.div(e, 4)
    zl = lax.rem(e, 4)
    return core, x, y, zh, zl


def device(core, x, y, z):
    return ((lax.div(z, 4) * 4 + x) * 2 + core, y * 4 + lax.rem(z, 4))


def one(v):
    return v + 1 - 2 * lax.rem(v, 2)


def two(v):
    return lax.rem(v + 2, 4)


def three(v):
    return 3 - v


def choose(i, table):
    value = table[0]
    for n in range(1, len(table)):
        value = jnp.where(i == n, table[n], value)
    return value


def swap(core, first, second):
    return first + core * (second - first), second + core * (first - second)


class Net:
    def __init__(self, send_sems, recv_sems):
        self.send_sems, self.recv_sems = send_sems, recv_sems
        self.count = 0
        self.sent = []

    def make(self, src, dst, dev):
        index = self.count
        self.count += 1
        return pltpu.make_async_remote_copy(
            src_ref=src,
            dst_ref=dst,
            send_sem=self.send_sems.at[index],
            recv_sem=self.recv_sems.at[index],
            device_id=dev,
            device_id_type=MESH,
        )

    def plan(self, src, dst, dev):
        copy = self.make(src, dst, dev)
        self.sent.append(copy)
        return copy

    def send(self, src, dst, dev):
        copy = self.plan(src, dst, dev)
        copy.start()
        return copy

    def drain(self):
        for copy in self.sent:
            copy.wait_send()


class Later:
    def __init__(self, **kwargs):
        self.kwargs = kwargs

    def start(self):
        pltpu.make_async_remote_copy(**self.kwargs).start()

    def wait_recv(self):
        pltpu.make_async_remote_copy(**self.kwargs).wait_recv()

    def wait_send(self):
        pltpu.make_async_remote_copy(**self.kwargs).wait_send()


def greet(peers, meanwhile):
    barrier = pltpu.get_barrier_semaphore()
    for peer in peers:
        pl.semaphore_signal(barrier, inc=1, device_id=peer, device_id_type=MESH)
    meanwhile()
    pl.semaphore_wait(barrier, len(peers))


class Layer:
    def __init__(self, refs, net):
        self.__dict__.update(refs)
        self.net = net
        self.core, self.x, self.y, self.zh, self.zl = coords()
        self.z = self.zh * 4 + self.zl
        self.e = self.y * 4 + self.zl
        self.a, self.b = swap(self.core, self.y, self.x)
        core, x, y, z = self.core, self.x, self.y, self.z
        z_far = (1 - self.zh) * 4 + self.zl
        self.partner = device(1 - core, x, y, z)
        self.x_peers = [device(core, lax.rem(x + d, 4), y, z) for d in range(1, 4)]
        self.y_peers = [device(core, x, lax.rem(y + d, 4), z) for d in range(1, 4)]
        self.z_peers = [device(core, x, y, lax.rem(z + d, 8)) for d in range(1, 8)]
        self.far_peers = [device(core, lax.rem(x + d, 4), y, z_far) for d in range(4)]

    def place(self, a_, b_, z_):
        y_, x_ = swap(self.core, a_, b_)
        return device(self.core, x_, y_, z_)

    def load(self, src, dst):
        copy = pltpu.make_async_copy(src, dst, self.local_sems.at[self.loads])
        self.loads += 1
        copy.start()
        return copy

    def start(self):
        self.loads = 0
        core, x, y, zh, zl = self.core, self.x, self.y, self.zh, self.zl
        me = zh * 4 + x
        own_cache = self.load(self.cache, self.cached.at[zh, x, core])
        own_fresh = self.load(self.fresh, self.newer.at[zh, x, core])
        self.own_rows = self.load(
            self.residual.at[:, pl.ds(pl.multiple_of(me * 896, 128), 896)], self.rows_in.at[me]
        )
        self.uv_load = self.load(self.w_uv, self.uv)
        self.wo_load = self.load(
            self.w_out, self.wo.at[pl.ds(pl.multiple_of(core * 448, 64), 448)]
        )
        self.moe_loads = [
            self.load(self.w_gate, self.w_all.at[0]),
            self.load(self.w_up, self.w_all.at[1]),
            self.load(self.w_down, self.wd.at[0]),
        ]
        peers = self.x_peers + self.y_peers + self.z_peers + self.far_peers[1:] + [self.partner]
        greet(peers, self.prepare_queries)
        own_cache.wait()
        own_fresh.wait()

    def prepare_queries(self):
        x, y, zh, zl = self.x, self.y, self.zh, self.zl
        lane = lax.broadcasted_iota(jnp.int32, (1, 128), 1)
        marks = jnp.zeros((1, 128), F32)
        for j in range(4):
            for n in range(8):
                marks += jnp.where(lane == self.ids[j, n] + 16 * j, 1.0, 0.0)
        self.marks[zh, x, y, zl] = marks
        @pl.loop(0, 8)
        def _(i):
            some = pl.ds(pl.multiple_of(i * 8, 8), 8)
            rows = pl.ds(pl.multiple_of(i * 64, 64), 64)
            self.q[rows, 0:512] = self.q_nope[some].astype(F32).reshape(64, 512).astype(BF16)

        for h in range(8):
            self.pe[pl.ds(h, 64, stride=8), 0:64] = self.q_rope[:, h * 64 : h * 64 + 64].astype(F32)
        self.q[:, 512:576] = self.pe[:, 0:64].astype(BF16)
        self.peak[...] = jnp.full((512, 128), -jnp.inf, F32)
        self.mass[...] = jnp.zeros((512, 128), F32)
        self.mean[...] = jnp.zeros((4, 512, 128), F32)
    def gather_and_attend(self):
        net = self.net
        core, x, y, zh, zl, z = self.core, self.x, self.y, self.zh, self.zl, self.z
        far = 1 - zh
        x1, x2, x3 = one(x), two(x), three(x)
        to_one, to_three = device(core, x1, y, z), device(core, x3, y, z)
        parts = ((self.cached, 0, 288), (self.cached, 288, 288), (self.newer, 0, 64))

        def whole(side, column, dev):
            refs = [r.at[side, column, core, pl.ds(at, size)] for r, at, size in parts]
            return [net.plan(ref, ref, dev) for ref in refs]

        def piece(side, column, late, dev):
            refs = [
                r.at[side, column, core, pl.ds(at + late * size // 2, size // 2)] for r, at, size in parts
            ]
            return [net.plan(ref, ref, dev) for ref in refs]

        def go(copies):
            for copy in copies:
                copy.start()

        def arrive(copies):
            for copy in copies:
                copy.wait_recv()

        edge = jnp.logical_or(zl == 0, zl == 3)
        z_out = lax.rem(z + 8 + jnp.where(zl == 0, -1, 1), 8)
        z_in = lax.rem(z + 8 + jnp.where(zl == 0, 1, -1), 8)
        z_copies, z_nexts = [], []
        for r, at, size in parts:
            near_ref = r.at[zh, x, core, pl.ds(at, size)]
            far_ref = r.at[far, x, core, pl.ds(at, size)]
            z_copies.append(net.make(near_ref, near_ref, device(core, x, y, z_out)))
            z_nexts.append(net.make(far_ref, far_ref, device(core, x, y, z_in)))

        @pl.when(edge)
        def _():
            for copy in z_copies:
                copy.start()

        near = whole(zh, x, to_one), whole(zh, x, to_three)
        near_pieces = piece(zh, x1, 0, to_three), piece(zh, x3, 1, to_one)
        share = whole(far, x, to_one), whole(far, x, to_three)
        far_pieces = piece(far, x1, 0, to_three), piece(far, x3, 1, to_one)
        gifts = [whole(side, c, self.partner) for side in (zh, far) for c in (x, x1, x3, x2)]
        go(near[0] + near[1] + gifts[0])
        row_copies = []
        me = zh * 4 + x
        for d in range(7):
            column, side = lax.rem(x + (d + 1) % 4, 4), zh if d < 3 else far
            there = side * 4 + column
            row_copies.append(
                net.send(
                    self.residual.at[:, pl.ds(pl.multiple_of(there * 896, 128), 896)],
                    self.rows_in.at[me],
                    device(core, column, y, side * 4 + zl),
                )
            )
        mark = self.marks.at[zh, x, y, zl]
        marks_z = [net.send(mark, mark, p) for p in self.z_peers]
        mark = self.marks.at[:, x, y]
        marks_x = [net.plan(mark, mark, p) for p in self.x_peers]
        mark = self.marks.at[:, :, y]
        marks_y = [net.plan(mark, mark, p) for p in self.y_peers]
        wo_here = self.wo.at[pl.ds(pl.multiple_of(core * 448, 64), 448)]
        weights = [
            net.plan(self.w_out, wo_here, self.partner),
            net.plan(self.w_gate, self.w_all.at[2], self.partner),
            net.plan(self.w_up, self.w_all.at[3], self.partner),
            net.plan(self.w_down, self.wd.at[1], self.partner),
        ]

        order, first = self.order, core + 2 * me

        def pick(index, length, table):
            out = jnp.zeros(index.shape, jnp.int32)
            for n in range(length):
                out += jnp.where(index == n, order[table + n], 0)
            return out

        @pl.loop(0, 8)
        def _(i):
            @pl.when(i == 0)
            def _():
                arrive(gifts[0])

            @pl.when(i == 1)
            def _():
                for n in range(3):
                    for m in range(2):
                        near[m][n].wait_recv()
                        go([near_pieces[m][n], gifts[1 + m][n]])

                    @pl.when(edge)
                    def _():
                        z_copies[n].wait_recv()
                        z_nexts[n].start()

                arrive(gifts[1])

            @pl.when(i == 2)
            def _():
                arrive(marks_z)
                go(marks_x)
                arrive(gifts[2])

            @pl.when(i == 3)
            def _():
                for n in range(3):
                    @pl.when(jnp.logical_not(edge))
                    def _():
                        z_nexts[n].wait_recv()

                    go([share[0][n], share[1][n], gifts[4][n]])
                arrive(near_pieces[0] + near_pieces[1])
                go(gifts[3])
                arrive(gifts[3])

            @pl.when(i == 4)
            def _():
                arrive(marks_x)
                go(marks_y)
                arrive(gifts[4])

            @pl.when(i == 5)
            def _():
                for n in range(3):
                    for m in range(2):
                        share[m][n].wait_recv()
                        go([far_pieces[m][n], gifts[5 + m][n]])
                arrive(gifts[5])

            @pl.when(i == 6)
            def _():
                arrive(gifts[6])

            @pl.when(i == 7)
            def _():
                arrive(far_pieces[0] + far_pieces[1])
                go(gifts[7] + weights)
                arrive(gifts[7])

            with jax.named_scope("p_block"):
                side = jnp.where(i < 4, zh, far)
                j = lax.rem(i, 4)
                column = jnp.where(j == 0, x, jnp.where(j == 1, x1, jnp.where(j == 2, x3, x2)))
                old = jnp.concatenate([self.cached[side, column, 0], self.cached[side, column, 1]], axis=1)
                new = self.newer[side, column].reshape(128, 576)
                last = (((1,), (1,)), ((), ()))
                self.score[:, 0:256] = jnp.dot(self.q[...], old, preferred_element_type=F32)
                self.score[:, 256:384] = lax.dot_general(self.q[...], new, last, preferred_element_type=F32)
                lane = lax.broadcasted_iota(jnp.int32, (1, 128), 1)
                table = (side * 4 + column) * 4
                key_pos = pick(lax.div(lane, 32), 4, table) * 32 + lax.rem(lane, 32)

                @pl.loop(0, 512 // ROWS)
                def _(r):
                    here = pl.ds(pl.multiple_of(r * ROWS, ROWS), ROWS)
                    row = r * ROWS + lax.broadcasted_iota(jnp.int32, (ROWS, 1), 0)
                    first_pos, last_pos = order[first * 2] * 32, order[first * 2 + 1] * 32
                    pos = jnp.where(row < 256, first_pos, last_pos) + lax.rem(lax.div(row, 8), 32)
                    parts = [self.score[here, n * 128 : n * 128 + 128] * LOG_SCALE for n in range(3)]
                    parts[2] = jnp.where(key_pos <= pos, parts[2], -jnp.inf)
                    before = self.peak[here]
                    top = jnp.maximum(jnp.maximum(parts[0], parts[1]), parts[2])
                    peak = jnp.maximum(before, jnp.max(top, axis=1, keepdims=True))
                    fade = jnp.exp2(before - peak)
                    self.peak[here] = peak
                    self.fade[here] = fade
                    parts = [jnp.exp2(part - peak) for part in parts]
                    self.mass[here] = self.mass[here] * fade + (parts[0] + parts[1] + parts[2])
                    for n in range(3):
                        self.weight[here, n * 128 : n * 128 + 128] = parts[n].astype(BF16)

                added = lax.dot_general(
                    self.weight[:, 0:256], old[:512], last, preferred_element_type=F32
                ) + jnp.dot(self.weight[:, 256:384], new[:, :512], preferred_element_type=F32)
                for n in range(4):
                    self.mean[n] = self.mean[n] * self.fade[...] + added[:, n * 128 : n * 128 + 128]

        self.row_copies, self.weights, self.marks_y = row_copies, weights, marks_y
        self.edge, self.z_sent = edge, z_copies + z_nexts
        with jax.named_scope("p_values"):
            self.uv_load.wait()
            for h in range(8):
                some = pl.ds(h, 64, stride=8)
                mass = jnp.sum(self.mass[some], axis=1, keepdims=True)
                latent = jnp.concatenate([self.mean[n, some] / mass for n in range(4)], axis=1)
                high = latent.astype(BF16)
                low = (latent - high.astype(F32)).astype(BF16)
                out = jnp.dot(high, self.uv[h], preferred_element_type=F32)
                out += jnp.dot(low, self.uv[h], preferred_element_type=F32)
                self.heads[zh, x, :, h * 128 : h * 128 + 128] = out.astype(BF16)

    def prepare(self):
        for copy in [self.own_rows, self.wo_load]:
            copy.wait()
        for copy in self.row_copies + self.weights[:1] + self.marks_y:
            copy.wait_recv()
        self.rows[...] = jnp.zeros((128, 896), BF16)
        for block in range(8):
            self.rows[block * 16 : block * 16 + 4] = self.rows_in[block]

        @pl.loop(0, 128)
        def _(o):
            oy, oz = lax.div(lax.rem(o, 16), 4), lax.rem(o, 4)
            self.owners[pl.ds(o, 1)] = self.marks[lax.div(o, 64), lax.rem(lax.div(o, 16), 4), oy, oz]

        self.total[...] = jnp.zeros_like(self.total)
        self.logit[...] = jnp.zeros_like(self.logit)
        self.square[...] = jnp.zeros_like(self.square)

    def project_and_gather(self):
        net = self.net
        core, x, y, zh, zl, z, e = self.core, self.x, self.y, self.zh, self.zl, self.z, self.e
        a, b, place = self.a, self.b, self.place
        z_peers, z_far = self.z_peers, (1 - self.zh) * 4 + self.zl
        x1, x3 = one(x), three(x)
        to_one, to_three = device(core, x1, y, z), device(core, x3, y, z)

        cuts = pl.ds(0, 32), pl.ds(32, 32)
        x_sides = to_one, to_three

        def fan_out(side, half):
            ref = self.heads.at[side, x, cuts[half]]
            first = net.send(ref, ref, x_sides[half])
            second = net.send(ref, ref, x_sides[1 - half])
            return (first, second) if half == 0 else (second, first)

        def forward(side, copies):
            passed = []
            for half in range(2):
                copies[half][half].wait_recv()
                ref = self.heads.at[side, (x1, x3)[half], cuts[half]]
                passed.append(net.send(ref, ref, x_sides[1 - half]))
            return passed

        def arrive(side, copies, passed):
            copies[0][1].wait_recv()
            copies[1][0].wait_recv()
            for copy in passed:
                copy.wait_recv()

        def project(side):
            row = lax.broadcasted_iota(jnp.int32, (256, 128), 0) + side * 256
            col = lax.broadcasted_iota(jnp.int32, (256, 128), 1)
            pick = (row == lax.div(col, 16) * 64 + e * 4 + lax.rem(col, 16)) & (lax.rem(col, 16) < 4)
            pick = jnp.where(pick, 1.0, 0.0).astype(BF16)
            lhs = self.heads[side].reshape(256, 1024)
            for start, width in ((0, 256), (256, 256), (512, 256), (768, 128)):
                cols = pl.ds(start, width)
                block = lax.dot_general(
                    lhs, self.wo[cols], (((1,), (1,)), ((), ())), preferred_element_type=F32
                )
                block += jnp.dot(pick, self.rows[:, cols], preferred_element_type=F32)
                self.part[pl.ds(side * 2, 2), :, :, cols] = block.astype(BF16).reshape(2, 4, 32, width)

        with jax.named_scope("p_heads"):
            far_copies = []
            for half in range(2):
                ref = self.heads.at[zh, x, cuts[half]]
                far_copies.append(net.send(ref, ref, device(core, x, y, z_far)))
            near = fan_out(zh, 0), fan_out(zh, 1)
            self.prepare()
            near_passed = forward(zh, near)
            far = []
            for half in range(2):
                far_copies[half].wait_recv()
                far.append(fan_out(1 - zh, half))
        with jax.named_scope("p_near"):
            arrive(zh, near, near_passed)
            project(zh)
        with jax.named_scope("p_far"):
            far_passed = forward(1 - zh, far)
            arrive(1 - zh, far, far_passed)
            project(1 - zh)

        y1, y2, y3 = one(y), two(y), three(y)
        up, down = device(core, x, y1, z), device(core, x, y3, z)
        lo, hi = pl.ds(0, 2), pl.ds(2, 2)
        with jax.named_scope("p_sum_y"):
            s10 = net.send(self.part.at[y2, lo], self.y_in.at[0, 0], up)
            s20 = net.send(self.part.at[y2, hi], self.y_in.at[1, 0], down)
            s11 = net.send(self.part.at[y1, lo], self.y_in.at[0, 1], up)
            s21 = net.send(self.part.at[y3, hi], self.y_in.at[1, 1], down)
            s10.wait_recv()
            self.part[y3, lo] = (self.part[y3, lo].astype(F32) + self.y_in[0, 0].astype(F32)).astype(BF16)
            t1 = net.send(self.part.at[y3, lo], self.y_last.at[0], down)
            s20.wait_recv()
            self.part[y1, hi] = (self.part[y1, hi].astype(F32) + self.y_in[1, 0].astype(F32)).astype(BF16)
            t2 = net.send(self.part.at[y1, hi], self.y_last.at[1], up)
            s11.wait_recv()
            t1.wait_recv()
            self.part[y, lo] = (
                self.part[y, lo].astype(F32) + self.y_in[0, 1].astype(F32) + self.y_last[0].astype(F32)
            ).astype(BF16)
            s21.wait_recv()
            t2.wait_recv()
            self.part[y, hi] = (
                self.part[y, hi].astype(F32) + self.y_in[1, 1].astype(F32) + self.y_last[1].astype(F32)
            ).astype(BF16)
        with jax.named_scope("p_sum_z"):
            line = []
            for d in range(1, 4):
                there = lax.rem(zl + d, 4)
                line.append(
                    net.send(self.part.at[y, there], self.z_parts.at[d - 1], device(core, x, y, zh * 4 + there))
                )
            for copy in line:
                copy.wait_recv()
            hidden = self.part[y, zl].astype(F32)
            for d in range(3):
                hidden += self.z_parts[d].astype(F32)
            self.buf[a, b, z] = hidden[:, :768].astype(BF16)
        self.slim[z, a, b] = hidden[:, 768:].astype(BF16)

        with jax.named_scope("p_gather"):
            self.gather_rows()

    def gather_rows(self):
        net = self.net
        core, z = self.core, self.z
        a, b, place = self.a, self.b, self.place
        a1, a2, a3 = one(a), two(a), three(a)
        b1, b2, b3 = one(b), two(b), three(b)
        a_one, a_three = place(a1, b, z), place(a3, b, z)
        b_one, b_three = place(a, b1, z), place(a, b3, z)
        front, back = pl.ds(0, 4), pl.ds(4, 4)
        ref = self.buf.at[a, b, z]
        low, high = pl.ds(0, 16), pl.ds(16, 16)
        slim = self.slim
        slim_b = [net.send(slim.at[z, a, b], slim.at[z, a, b], p) for p in (b_one, b_three)]
        by_z = {d: net.send(ref, ref, self.z_peers[d - 1]) for d in (2, 6, 1, 7)}

        def fan(z_):
            ref = self.buf.at[a, b, z_]
            return [net.send(ref, ref, p) for p in (b_one, b_three, a_one, a_three)]

        def farther(d, hop, rows):
            by_z[d].wait_recv()
            z_ = lax.rem(z + 8 - d, 8)
            ref, part = self.buf.at[a, b, z_], self.buf.at[a, b, z_, rows]
            return net.send(ref, ref, self.z_peers[hop - 1]), net.send(part, part, self.z_peers[2 * hop % 8 - 1])

        with jax.named_scope("p_fan"):
            fans = [fan(z)]
            slim_b[0].wait_recv()
            ref = slim.at[z, a, b1, low]
            slim_more = [net.send(ref, ref, b_three)]
            slim_b[1].wait_recv()
            ref = slim.at[z, a, b3, high]
            slim_more.append(net.send(ref, ref, b_one))
            by_z[3], low_half = farther(2, 1, low)
            by_z[5], high_half = farther(6, 7, high)
            for d in (1, 7):
                by_z[d].wait_recv()
                fans.append(fan(lax.rem(z + 8 - d, 8)))
            for copy in slim_more:
                copy.wait_recv()
            ref = slim.at[z, a]
            slim_a = [net.send(ref, ref, p) for p in (a_one, a_three)]
            fans.append(fan(lax.rem(z + 6, 8)))
            fans.append(fan(lax.rem(z + 2, 8)))
            for d in (3, 5):
                by_z[d].wait_recv()
                fans.append(fan(lax.rem(z + 8 - d, 8)))
            low_half.wait_recv()
            high_half.wait_recv()
            fans.append(fan(lax.rem(z + 4, 8)))
            refs = slim.at[z, a1, pl.ds(0, 2)], slim.at[z, a3, pl.ds(2, 2)]
            slim_halves = [net.plan(ref, ref, dev) for ref, dev in zip(refs, (a_three, a_one))]
            slim_z = {d: net.plan(slim.at[z], slim.at[z], self.z_peers[d - 1]) for d in (2, 6, 1, 7)}
            slim_far = {}
            for d, hop, late in ((2, 1, 0), (6, 7, 2)):
                z_ = lax.rem(z + 8 - d, 8)
                part = slim.at[z_, pl.ds(late, 2)]
                slim_far[d] = (
                    net.plan(slim.at[z_], slim.at[z_], self.z_peers[hop - 1]),
                    net.plan(part, part, self.z_peers[2 * hop % 8 - 1]),
                )

        def spread(column):
            ref = self.buf.at[a, column]
            return [net.plan(ref, ref, p) for p in (a_one, a_three)]

        def halves(column):
            ref, other = self.buf.at[a1, column, front], self.buf.at[a3, column, back]
            return [net.plan(ref, ref, a_three), net.plan(other, other, a_one)]

        ref, other = self.buf.at[a, b1, front], self.buf.at[a, b3, back]
        b_halves = [net.plan(ref, ref, b_three), net.plan(other, other, b_one)]
        columns = (b, b1, b3, b2)
        spreads = [None] + [spread(column) for column in columns[1:]]
        passed = [halves(column) for column in columns]

        def go(*copies):
            for copy in copies:
                copy.start()

        def arrive(*copies):
            for copy in copies:
                copy.wait_recv()

        def pass_on(n):
            if n == 0:
                arrive(*[f[2] for f in fans])
                go(passed[0][0])
                arrive(*[f[3] for f in fans])
                go(passed[0][1])
            else:
                arrive(spreads[n][0])
                go(passed[n][0])
                arrive(spreads[n][1])
                go(passed[n][1])

        def first_sides():
            arrive(*slim_halves)
            go(*slim_z.values())
            arrive(*[f[0] for f in fans])
            go(b_halves[0], *spreads[1])
            arrive(*[f[1] for f in fans])
            go(b_halves[1], *spreads[2])

        def far_column():
            arrive(*b_halves)
            go(*spreads[3])
            for d in (2, 6):
                arrive(slim_z[d])
                go(*slim_far[d])

        def slim_products():
            arrive(slim_z[1], slim_z[7], *slim_far[2], *slim_far[6])

            @pl.loop(0, 8)
            def _(z_):
                side, row_z = lax.div(z_, 4), lax.rem(z_, 4)
                columns, weights, gains, routers = [], [], [], []
                for col_x in range(4):
                    features = pl.ds(pl.multiple_of((side * 4 + col_x) * 896 + 768, 128), 128)
                    rows = []
                    for row_y in range(4):
                        aa, bb = swap(core, row_y, col_x)
                        rows.append(slim[z_, aa, bb])
                    columns.append(jnp.concatenate(rows, axis=0))
                    weights.append(jnp.concatenate([self.w_all[n, features] for n in range(4)], axis=1))
                    gains.append(self.gain[:, features])
                    routers.append(self.router[:, features])
                piece = jnp.concatenate(columns, axis=1).astype(F32)
                square = jnp.sum(piece * piece, axis=1, keepdims=True)
                scaled = (piece * jnp.concatenate(gains, axis=1)).astype(BF16)
                total = jnp.dot(scaled, jnp.concatenate(weights, axis=0), preferred_element_type=F32)
                logit = lax.dot_general(
                    scaled, jnp.concatenate(routers, axis=1), (((1,), (1,)), ((), ())),
                    preferred_element_type=F32,
                )
                for row_y in range(4):
                    here = pl.ds(pl.multiple_of(row_y * 128 + row_z * 32, 32), 32)
                    some = slice(row_y * 32, row_y * 32 + 32)
                    self.square[here] += jnp.broadcast_to(square[some], (32, 128))
                    self.total[here] += total[some]
                    self.logit[here] += logit[some]

            arrive(*passed[1])

        def weights_here():
            for n in range(2):
                slim_a[n].wait_recv()
                slim_halves[n].start()
            for load in self.moe_loads:
                load.wait()
            for copy in self.weights[1:]:
                copy.wait_recv()

        steps = {
            0: weights_here,
            1: first_sides,
            3: lambda: pass_on(0),
            5: far_column,
            6: lambda: pass_on(1),
            8: lambda: arrive(*passed[0]),
            9: lambda: pass_on(2),
            11: slim_products,
            12: lambda: pass_on(3),
            14: lambda: arrive(*passed[2]),
            15: lambda: arrive(*passed[3]),
        }
        order_a = (a, a, a, a1, a3, a, a1, a3, a2, a1, a3, a2, a1, a3, a2, a2)
        order_b = (b, b1, b3, b, b, b2, b1, b1, b, b3, b3, b1, b2, b2, b3, b2)

        @pl.loop(0, 16)
        def _(i):
            for n, step in steps.items():
                pl.when(i == n)(step)
            with jax.named_scope("p_unit"):
                aa, bb = choose(i, order_a), choose(i, order_b)
                row_y, col_x = swap(core, aa, bb)
                here = pl.ds(pl.multiple_of(row_y * 128, 128), 128)
                for side in range(2):
                    features = pl.ds(pl.multiple_of((side * 4 + col_x) * 896, 128), 768)
                    piece = self.buf[aa, bb, pl.ds(side * 4, 4)].reshape(128, 768).astype(F32)
                    self.square[here] += jnp.broadcast_to(
                        jnp.sum(piece * piece, axis=1, keepdims=True), (128, 128)
                    )
                    scaled = (piece * self.gain[:, features]).astype(BF16)
                    weights = jnp.concatenate([self.w_all[n, features] for n in range(4)], axis=1)
                    self.total[here] += jnp.dot(scaled, weights, preferred_element_type=F32)
                    self.logit[here] += lax.dot_general(
                        scaled, self.router[:, features], (((1,), (1,)), ((), ())),
                        preferred_element_type=F32,
                    )

    def experts(self):
        core, e = self.core, self.e

        @pl.loop(0, 2)
        def _(side):
            here = pl.ds(pl.multiple_of(side * 256, 256), 256)
            scale = lax.rsqrt(self.square[here] * (1.0 / 7168.0) + NORM_EPS)
            row = lax.broadcasted_iota(jnp.int32, (256, 128), 0)
            col = lax.broadcasted_iota(jnp.int32, (256, 128), 1)
            owner = jnp.where(col == side * 64 + lax.div(row, 4), 1.0, 0.0)
            named = jnp.dot(owner, self.owners[...], preferred_element_type=F32)
            mask = jnp.zeros((256, 16), F32)
            for n in range(4):
                mask += jnp.where(lax.rem(row[:, :16], 4) == n, named[:, n * 16 : n * 16 + 16], 0.0)
            chosen = mask * jax.nn.sigmoid(self.logit[here] * scale[:, :16])
            lane = lax.broadcasted_iota(jnp.int32, (256, 16), 1)
            named = jnp.sum(jnp.where(lane == e, chosen, 0.0), axis=1, keepdims=True)
            mix = ROUTE_SCALE * named / jnp.sum(chosen, axis=1, keepdims=True)
            for i in range(2):
                gate = self.total[here, i * 256 : i * 256 + 128] * scale
                upward = self.total[here, i * 256 + 128 : i * 256 + 256] * scale
                act = (gate * jax.nn.sigmoid(gate) * upward * mix).astype(BF16)
                act = act.reshape(4, 4, 16, 128)
                for bx in range(4):
                    for by in range(4):
                        aa, bb = swap(core, by, bx)
                        self.act[aa, bb, side, :, i * 128 : i * 128 + 128] = act[bx, by]

    def own_hidden(self):
        owner = (self.zh * 4 + self.x) * 2 + lax.div(self.e, 8)
        oy, oz = lax.div(owner, 4), lax.rem(owner, 4)
        row = lax.broadcasted_iota(jnp.int32, (16, 32), 0)
        col = lax.broadcasted_iota(jnp.int32, (16, 32), 1)
        mine = jnp.where((col == lax.rem(self.e, 8) * 4 + row) & (row < 4), 1.0, 0.0).astype(BF16)
        for block in range(8):
            aa, bb = swap(self.core, oy, block % 4)
            rows = self.buf[aa, bb, block // 4 * 4 + oz]
            self.own[:, block * 896 : block * 896 + 768] = jnp.dot(
                mine, rows, preferred_element_type=F32
            )
            rows = self.slim[block // 4 * 4 + oz, aa, bb]
            self.own[:, block * 896 + 768 : block * 896 + 896] = jnp.dot(
                mine, rows, preferred_element_type=F32
            )

    def mix_down(self):
        net = self.net
        z = self.z
        a, b, place = self.a, self.b, self.place
        a1, a2, a3 = one(a), two(a), three(a)
        b1, b2, b3 = one(b), two(b), three(b)
        a_up, a_down = place(a1, b, z), place(a3, b, z)
        b_up, b_down = place(a, b1, z), place(a, b3, z)
        base, each = net.count, 19
        net.count += each * CHUNKS

        def copies(g):
            found = []

            def add(src, dst, dev):
                index = base + g * each + len(found)
                found.append(Later(
                    src_ref=src, dst_ref=dst, send_sem=net.send_sems.at[index],
                    recv_sem=net.recv_sems.at[index], device_id=dev, device_id_type=MESH,
                ))

            add(self.prod.at[0, g, a2], self.a_in.at[0, g, 0], a_up)
            add(self.prod.at[1, g, a2], self.a_in.at[1, g, 0], a_down)
            add(self.prod.at[0, g, a1], self.a_in.at[0, g, 1], a_up)
            add(self.prod.at[1, g, a3], self.a_in.at[1, g, 1], a_down)
            add(self.prod.at[0, g, a3], self.a_last.at[0, g], a_down)
            add(self.prod.at[1, g, a1], self.a_last.at[1, g], a_up)
            add(self.prod.at[0, g, a, b2], self.b_in.at[0, g, 0], b_up)
            add(self.prod.at[1, g, a, b2], self.b_in.at[1, g, 0], b_down)
            add(self.prod.at[0, g, a, b1], self.b_in.at[0, g, 1], b_up)
            add(self.prod.at[1, g, a, b3], self.b_in.at[1, g, 1], b_down)
            add(self.prod.at[0, g, a, b3], self.b_last.at[0, g], b_down)
            add(self.prod.at[1, g, a, b1], self.b_last.at[1, g], b_up)
            for d in range(1, 8):
                add(self.pack.at[g, d], self.z_in.at[g, d - 1], self.z_peers[d - 1])
            return found

        def merge(half, g, index, *sources):
            @pl.loop(0, 4)
            def _(r):
                value = self.prod[half, g, index, r].astype(F32)
                for source in sources:
                    value += source[r].astype(F32)
                self.prod[half, g, index, r] = value.astype(BF16)

        def add_in(half, g, index, *sources):
            value = self.prod[half, g, a, index].astype(F32)
            for source in sources:
                value += source[...].astype(F32)
            self.prod[half, g, a, index] = value.astype(BF16)

        def products(g):
            c = copies(g)

            @pl.loop(0, 8)
            def _(n):
                half = lax.rem(n, 2)
                index = choose(n, (a2, a2, a1, a3, a3, a1, a, a))
                cols = pl.ds(pl.multiple_of(half * 3584 + g * 512, 512), 512)
                block = jnp.dot(
                    self.act[index].reshape(128, 256), self.wd[:, :, cols].reshape(256, 512),
                    preferred_element_type=F32,
                )
                self.prod[half, g, index] = block.astype(BF16).reshape(4, 32, 512)
                for k in range(4):
                    pl.when(n == k)(c[k].start)

        def second(g):
            c = copies(g)
            c[0].wait_recv()
            merge(0, g, a3, self.a_in.at[0, g, 0])
            c[4].start()
            c[1].wait_recv()
            merge(1, g, a1, self.a_in.at[1, g, 0])
            c[5].start()

        def third(g):
            c = copies(g)
            c[2].wait_recv()
            c[4].wait_recv()
            merge(0, g, a, self.a_in.at[0, g, 1], self.a_last.at[0, g])
            c[6].start()
            c[8].start()
            c[3].wait_recv()
            c[5].wait_recv()
            merge(1, g, a, self.a_in.at[1, g, 1], self.a_last.at[1, g])
            c[7].start()
            c[9].start()

        def fourth(g):
            c = copies(g)
            c[6].wait_recv()
            add_in(0, g, b3, self.b_in.at[0, g, 0])
            c[10].start()
            c[7].wait_recv()
            add_in(1, g, b1, self.b_in.at[1, g, 0])
            c[11].start()

        def fifth(g):
            c = copies(g)
            c[8].wait_recv()
            c[10].wait_recv()
            add_in(0, g, b, self.b_in.at[0, g, 1], self.b_last.at[0, g])
            c[9].wait_recv()
            c[11].wait_recv()
            add_in(1, g, b, self.b_in.at[1, g, 1], self.b_last.at[1, g])
            value = jnp.zeros((128, 256), F32)
            for q in range(4):
                rows = self.prod[q // 2, g, a, b, :, q % 2 * 256 : q % 2 * 256 + 256]
                value += jnp.dot(self.picks[q], rows, preferred_element_type=F32)
            self.pack[g] = value.astype(BF16).reshape(8, 16, 256)
            for d in range(7):
                c[12 + d].start()

        def last(g):
            c = copies(g)
            result = self.pack[g, 0].astype(F32)
            for d in range(7):
                c[12 + d].wait_recv()
                result += self.z_in[g, d].astype(F32)
            for q in range(4):
                start = q // 2 * 3584 + q % 2 * 256 + g * 512
                cols = pl.ds(pl.multiple_of(start, 256), 256)
                self.out[:, cols] = (result[q * 4 : q * 4 + 4] + self.own[0:4, cols]).astype(BF16)
            for copy in c:
                copy.wait_send()

        v = {}
        ups = (a_up, a_down)
        b_peers = [place(a, lax.rem(b + d, 4), z) for d in range(1, 4)]
        v["z"] = [net.plan(self.v_prod.at[d], self.v_z.at[d - 1], self.z_peers[d - 1]) for d in range(1, 8)]
        v["first"] = [
            net.plan(self.v_sum.at[half, index], self.v_a.at[half, n], ups[half])
            for half, n, index in ((0, 0, a2), (1, 0, a2), (0, 1, a1), (1, 1, a3))
        ]
        v["second"] = [
            net.plan(self.v_sum.at[half, index], self.v_last.at[half], ups[1 - half])
            for half, index in ((0, a3), (1, a1))
        ]
        v["b"] = [net.plan(self.v_pack.at[d], self.v_b.at[d - 1], b_peers[d - 1]) for d in range(1, 4)]

        def v_products():
            row = lax.broadcasted_iota(jnp.int32, (256, 256), 0)
            col = lax.broadcasted_iota(jnp.int32, (256, 256), 1)
            source = lax.rem(lax.div(row, 4), 16) * 16 + lax.div(row, 64) * 4 + lax.rem(row, 4)
            order = jnp.where(col == source, 1.0, 0.0).astype(BF16)
            for side in range(2):
                rows = jnp.dot(order, self.act[:, :, side].reshape(256, 256), preferred_element_type=F32)
                self.act_z[pl.ds(side * 4, 4)] = rows.astype(BF16).reshape(4, 64, 256)

            @pl.loop(0, 8)
            def _(n):
                d = choose(n, (4, 3, 5, 2, 6, 1, 7, 0))
                for half in range(2):
                    start = half * 3584 + CHUNKS * 512
                    block = jnp.dot(
                        self.act_z[lax.rem(z + d, 8)], self.wd[:, :, start : start + 512].reshape(256, 512),
                        preferred_element_type=F32,
                    )
                    self.v_prod[d, :, half * 512 : half * 512 + 512] = block.astype(BF16)
                for k in range(1, 8):
                    pl.when(d == k)(v["z"][k - 1].start)

        def v_first():
            for copy in v["z"]:
                copy.wait_recv()
            for half in range(2):
                cols = pl.ds(half * 512, 512)
                value = self.v_prod[0, :, cols].astype(F32)
                for d in range(7):
                    value += self.v_z[d, :, cols].astype(F32)
                self.v_sum[half] = value.astype(BF16).reshape(4, 16, 512)
            for copy in v["first"]:
                copy.start()

        def v_add(half, index, *sources):
            value = self.v_sum[half, index].astype(F32)
            for source in sources:
                value += source[...].astype(F32)
            self.v_sum[half, index] = value.astype(BF16)

        def v_second():
            for half, index in ((0, a3), (1, a1)):
                v["first"][half].wait_recv()
                v_add(half, index, self.v_a.at[half, 0])
                v["second"][half].start()

        def v_third():
            for half in range(2):
                v["first"][2 + half].wait_recv()
                v["second"][half].wait_recv()
                v_add(half, a, self.v_a.at[half, 1], self.v_last.at[half])
            row = lax.broadcasted_iota(jnp.int32, (64, 16), 0)
            col = lax.broadcasted_iota(jnp.int32, (64, 16), 1)
            there = lax.rem(b + lax.div(row, 16), 4)
            value = jnp.zeros((64, 256), F32)
            for q in range(4):
                hit = (col == there * 4 + lax.rem(row, 4)) & (lax.rem(lax.div(row, 4), 4) == q)
                hit = jnp.where(hit, 1.0, 0.0).astype(BF16)
                rows = self.v_sum[q // 2, a, :, q % 2 * 256 : q % 2 * 256 + 256]
                value += jnp.dot(hit, rows, preferred_element_type=F32)
            self.v_pack[...] = value.astype(BF16).reshape(4, 16, 256)
            for copy in v["b"]:
                copy.start()

        def v_finish():
            result = self.v_pack[0].astype(F32)
            for d in range(3):
                v["b"][d].wait_recv()
                result += self.v_b[d].astype(F32)
            for q in range(4):
                start = q // 2 * 3584 + q % 2 * 256 + CHUNKS * 512
                cols = slice(start, start + 256)
                self.out[:, cols] = (result[q * 4 : q * 4 + 4] + self.own[0:4, cols]).astype(BF16)

        row = lax.broadcasted_iota(jnp.int32, (128, 32), 0)
        col = lax.broadcasted_iota(jnp.int32, (128, 32), 1)
        there = lax.rem(z + lax.div(row, 16), 8)
        for q in range(4):
            hit = (col == there * 4 + lax.rem(row, 4)) & (lax.rem(lax.div(row, 4), 4) == q)
            self.picks[q] = jnp.where(hit, 1.0, 0.0).astype(BF16)
        stages = (products, second, third, fourth, fifth, last)

        @pl.loop(0, CHUNKS + len(stages) + 1)
        def _(t):
            for n, stage in enumerate(stages):
                g = t - n - 2 * (n // 5)

                @pl.when((g >= 0) & (g < CHUNKS))
                def _():
                    with jax.named_scope("p_stage%d" % n):
                        stage(g)

            @pl.when(t == 1)
            def _():
                with jax.named_scope("p_v0"):
                    v_products()
                self.own_hidden()

            for n, stage in enumerate((v_first, v_second, v_third, v_finish)):
                @pl.when(t == 6 + n)
                def _():
                    with jax.named_scope("p_v%d" % (n + 1)):
                        stage()

    def finish(self):
        @pl.when(self.edge)
        def _():
            for copy in self.z_sent:
                copy.wait_send()

        self.net.drain()


ANY = pl.BlockSpec(memory_space=pl.ANY)
VM = pl.BlockSpec(memory_space=pltpu.VMEM)
SM = pl.BlockSpec(memory_space=pltpu.SMEM)
DMA = pltpu.SemaphoreType.DMA
INPUTS = (
    ("q_nope", VM), ("q_rope", VM), ("cache", ANY), ("fresh", ANY), ("order", SM), ("w_uv", ANY),
    ("w_out", ANY), ("residual", ANY), ("gain", VM), ("router", VM), ("ids", SM), ("w_gate", ANY),
    ("w_up", ANY), ("w_down", ANY),
)
SCRATCH = (
    ("cached", (2, 4, 2, 576, 128), BF16),
    ("newer", (2, 4, 2, 64, 576), BF16),
    ("rows_in", (8, 4, 896), BF16),
    ("rows", (128, 896), BF16),
    ("marks", (2, 4, 4, 4, 1, 128), F32),
    ("owners", (128, 128), F32),
    ("uv", (8, 512, 128), BF16),
    ("wo", (896, 1024), BF16),
    ("w_all", (4, 7168, 128), BF16),
    ("wd", (2, 128, 7168), BF16),
    ("q", (512, 576), BF16),
    ("pe", (512, 128), F32),
    ("score", (512, 384), F32),
    ("weight", (512, 384), BF16),
    ("peak", (512, 128), F32),
    ("mass", (512, 128), F32),
    ("mean", (4, 512, 128), F32),
    ("fade", (512, 128), F32),
    ("heads", (2, 4, 64, 1024), BF16),
    ("part", (4, 4, 32, 896), BF16),
    ("y_in", (2, 2, 2, 32, 896), BF16),
    ("y_last", (2, 2, 32, 896), BF16),
    ("z_parts", (3, 32, 896), BF16),
    ("buf", (4, 4, 8, 32, 768), BF16),
    ("slim", (8, 4, 4, 32, 128), BF16),
    ("total", (512, 512), F32),
    ("logit", (512, 16), F32),
    ("square", (512, 128), F32),
    ("act", (4, 4, 2, 16, 256), BF16),
    ("own", (16, 7168), F32),
    ("prod", (2, CHUNKS, 4, 4, 32, 512), BF16),
    ("a_in", (2, CHUNKS, 2, 4, 32, 512), BF16),
    ("a_last", (2, CHUNKS, 4, 32, 512), BF16),
    ("b_in", (2, CHUNKS, 2, 32, 512), BF16),
    ("b_last", (2, CHUNKS, 32, 512), BF16),
    ("act_z", (8, 64, 256), BF16),
    ("v_prod", (8, 64, 1024), BF16),
    ("v_z", (7, 64, 1024), BF16),
    ("v_sum", (2, 4, 16, 512), BF16),
    ("v_a", (2, 2, 16, 512), BF16),
    ("v_last", (2, 16, 512), BF16),
    ("v_pack", (4, 16, 256), BF16),
    ("v_b", (3, 16, 256), BF16),
    ("picks", (4, 128, 32), BF16),
    ("pack", (CHUNKS, 8, 16, 256), BF16),
    ("z_in", (CHUNKS, 7, 16, 256), BF16),
)
COPIES = 400


def layer_kernel(*refs):
    names = [n for n, _ in INPUTS] + ["out"] + [n for n, *_ in SCRATCH]
    layer = Layer(dict(zip(names, refs)), Net(*refs[-2:]))
    layer.local_sems = refs[-3]
    with jax.named_scope("p_start"):
        layer.start()
    with jax.named_scope("p_attend"):
        layer.gather_and_attend()
    with jax.named_scope("p_project"):
        layer.project_and_gather()
    with jax.named_scope("p_experts"):
        layer.experts()
    with jax.named_scope("p_down"):
        layer.mix_down()
    layer.finish()


def body(
    q_nope, q_rope, cache_keys, fresh_keys, block_order, w_uv, w_out, residual,
    norm_gain, router_weight, expert_ids, w_gate, w_up, w_down,
):
    return pl.pallas_call(
        layer_kernel,
        out_shape=jax.ShapeDtypeStruct((4, 7168), BF16),
        in_specs=[spec for _, spec in INPUTS],
        out_specs=VM,
        scratch_shapes=[pltpu.VMEM(dims, kind) for _, dims, kind in SCRATCH]
        + [DMA((8,)), DMA((COPIES,)), DMA((COPIES,))],
        compiler_params=pltpu.CompilerParams(
            collective_id=0, has_side_effects=True, vmem_limit_bytes=VMEM_LIMIT
        ),
    )(
        q_nope, q_rope, cache_keys, fresh_keys.T, block_order, w_uv, w_out.T, residual,
        norm_gain.reshape(1, 7168), router_weight.T, expert_ids, w_gate[0], w_up[0], w_down[0],
    )


def solution(mesh):
    return jax.shard_map(
        body,
        mesh=mesh,
        in_specs=(
            P("ctx", "exp", None),
            P("ctx", "exp"),
            P(None, "ctx"),
            P(None, "ctx"),
            P(),
            P("exp", None, None),
            P("exp", "ctx"),
            P(("ctx", "exp"), None),
            P(),
            P(),
            P(("ctx", "exp"), None),
            P("exp", None, "ctx"),
            P("exp", None, "ctx"),
            P("exp", "ctx", None),
        ),
        out_specs=P(("ctx", "exp"), None),
        check_vma=False,
    )
```
